256 devices in a mesh: box: 256 (over y, z, x, core).
Axes of the slice: x: 4, y: 4, z: 8, core: 2. Of those that a mesh axis runs over, the one named last changes fastest.
Arguments:
- basis_vector: float32 [16, 1048576], P(None, 'box'), may hold values from -600 to 600
- diagonal: float32 [1048576], P('box'), may hold values from 0.25 to 2
- coords: int32 [2, 1048576], P(None, 'box'), may hold values from 0 to 4095
- phase_scale: int32 [1], replicated, may hold values from 1 to 8190
- sketch_rows: int32 [1048576], P('box'), may hold values from 0 to 2047
- sketch_signs: int32 [1048576], P('box'), may hold values from 0 to 1
Outputs:
- new_basis: float32 [16, 1048576], P(None, 'box')
- sketch: float32 [16, 2048], replicated
- arnoldi: float32 [2, 16], replicated
The draws below stay inside these ranges and needn't reach their ends.
All inputs are finite; a program needn't handle non-finite values.
Results may differ from the reference program's by a relative error of at most 0.00019.
Values sent between devices are 32-bit elements; how exact they have to be, the bound alone decides.
A program may use at most 64 MiB of HBM per device.

```python
import math
import jax
import jax.numpy as jnp
from jax import lax

RANK = 16
WIDTH = 32
LEAF = 32
GRID = 4096
SKETCH = 2048
NRHS = 16
BOX_DEV = 128
NPTS = 1048576
SECTIONS = 8
N_BOX = 256


def draw_basis_vector(key, part):
    key_scale, key_normal = jax.random.split(key, 2)
    position = jnp.arange(NPTS, dtype=jnp.float32) / NPTS
    row_scale = jnp.exp(jax.random.uniform(key_scale, (NPTS,), jnp.float32, 0.0, math.log(10.0))) * jnp.exp(position * math.log(3.0))
    normal_part = jax.random.normal(key_normal, (NRHS, NPTS), jnp.float32)
    return jnp.clip(normal_part, -4.0, 4.0) * row_scale[None, :]


def with_ends(drawn, own_key, low, largest):
    spot = [jax.random.randint(jax.random.fold_in(own_key, axis), (), 0, length) for axis, length in enumerate(drawn.shape)]
    widest = drawn.shape.index(max(drawn.shape))
    next_to = spot[:widest] + [(spot[widest] + 1) % drawn.shape[widest]] + spot[widest + 1:]
    return drawn.at[tuple(spot)].set(low).at[tuple(next_to)].set(largest)


def levels(own_key, shape, pieces, low, top_value):
    gain, own = 1.0, jax.random.fold_in(own_key, 6)
    for dim, shards_of in pieces:
        steps = jnp.exp(jax.random.uniform(jax.random.fold_in(own, dim), (shards_of,), jnp.float32, low / len(pieces), top_value / len(pieces)))
        gain = gain * jnp.repeat(steps, shape[dim] // shards_of).reshape([-1 if axis == dim else 1 for axis in range(len(shape))])
    return gain


def setup_inputs(seed: int = 0) -> dict:
    keys = jax.random.split(jax.random.key(seed), 7)
    basis_vector = draw_basis_vector(jax.random.fold_in(keys[6], 71), 0)
    diagonal = jnp.clip(jnp.exp(math.log(2.0) - 2.0794415 * jax.random.uniform(keys[1], (NPTS,), jnp.float32) ** levels(keys[1], (NPTS,), ((0, 256),), -0.2, 0.2)), 0.25, 2.0)
    coords = with_ends(jax.random.randint(keys[2], (2, NPTS), 0, GRID), jax.random.fold_in(keys[2], 1), 0, GRID - 1).astype(jnp.int32)
    phase_scale = jax.random.randint(keys[3], (1,), 1, 8191).astype(jnp.int32)
    sketch_rows = with_ends(jax.random.randint(keys[4], (NPTS,), 0, SKETCH), jax.random.fold_in(keys[4], 1), 0, SKETCH - 1).astype(jnp.int32)
    sketch_signs = with_ends(jax.random.randint(keys[5], (NPTS,), 0, 2), jax.random.fold_in(keys[5], 1), 0, 1).astype(jnp.int32)
    return {"basis_vector": basis_vector, "diagonal": diagonal, "coords": coords, "phase_scale": phase_scale, "sketch_rows": sketch_rows, "sketch_signs": sketch_signs}


modulus = 8191
epsilon = 1e-06

def leaf_table(coords, phase_scale):
    scale_mod = phase_scale[0] % modulus
    freq = jnp.arange(RANK, dtype=jnp.int32)
    freq_first = freq % 4 + 1
    freq_second = freq // 4 + 1
    linear = (freq_first[:, None] * coords[0][None, :] + freq_second[:, None] * coords[1][None, :]) % modulus
    phase = scale_mod * linear % modulus
    angle = phase.astype(jnp.float32) * (2.0 * math.pi / modulus)
    return jnp.concatenate([jnp.cos(angle), jnp.sin(angle)], 0) * (1.0 / math.sqrt(LEAF))

def translations(box_ids, segment_num, phase_scale):
    scale_mod = phase_scale[0] % modulus
    base_key = (box_ids * 37 + 101 * segment_num) % (modulus - 1) + 1
    unit_phase = scale_mod * base_key % modulus
    indices = jnp.arange(WIDTH, dtype=jnp.int32)
    prod_a = (indices[:, None] + 1) * (indices[None, :] + 2) % modulus
    prod_b = (indices[:, None] + 3) * (indices[None, :] + 1) % modulus
    phase_a = prod_a[:, :, None] * unit_phase[None, None, :] % modulus
    phase_b = (prod_b[:, :, None] * unit_phase[None, None, :] + 4096) % modulus
    factor = 2.0 * math.pi / modulus
    ident = jnp.eye(WIDTH, dtype=jnp.float32)[:, :, None]
    own_map = 0.85 * ident + 0.35 / math.sqrt(WIDTH) * jnp.cos(phase_a.astype(jnp.float32) * factor)
    cross_map = 0.6 / math.sqrt(WIDTH) * jnp.cos(phase_b.astype(jnp.float32) * factor)
    return (own_map, cross_map)

def reference(basis_vector, diagonal, coords, phase_scale, sketch_rows, sketch_signs):
    highest = lax.Precision.HIGHEST
    columns = basis_vector.shape[0]
    points = basis_vector.shape[1]
    box_count = points // LEAF
    leaf_map = leaf_table(coords, phase_scale)
    leaf_boxes = leaf_map.reshape(WIDTH, box_count, LEAF)
    blocks = basis_vector.reshape(columns, box_count, LEAF)
    coeffs = jnp.einsum('wbs,qbs->wqb', leaf_boxes, blocks, precision=highest)
    coeffs = coeffs.reshape(WIDTH, columns, N_BOX, BOX_DEV)
    box_ids = jnp.arange(box_count, dtype=jnp.int32)
    for segment_num in range(SECTIONS):
        stride = 2 ** segment_num
        grouped = coeffs.reshape(WIDTH, columns, N_BOX // (2 * stride), 2, stride, BOX_DEV)
        partner = grouped[:, :, :, ::-1].reshape(WIDTH, columns, N_BOX, BOX_DEV)
        own_map, cross_map = translations(box_ids, segment_num, phase_scale)
        own_map = own_map.reshape(WIDTH, WIDTH, N_BOX, BOX_DEV)
        cross_map = cross_map.reshape(WIDTH, WIDTH, N_BOX, BOX_DEV)
        coeffs = jnp.einsum('wvdg,vqdg->wqdg', own_map, coeffs, precision=highest) + jnp.einsum('wvdg,vqdg->wqdg', cross_map, partner, precision=highest)
    target_coef = coeffs.reshape(WIDTH, columns, box_count)
    applied = jnp.einsum('wbs,wqb->qbs', leaf_boxes, target_coef, precision=highest).reshape(columns, points)
    image = diagonal[None, :] * basis_vector + applied
    inner_vw = lax.optimization_barrier(jnp.mean(basis_vector * image, axis=1))
    square = lax.optimization_barrier(jnp.mean(basis_vector * basis_vector, axis=1)) + epsilon
    projection = inner_vw / square
    residual = image - projection[:, None] * basis_vector
    spread = jnp.sqrt(lax.optimization_barrier(jnp.mean(residual * residual, axis=1)) + epsilon)
    new_basis = residual / spread[:, None]
    sign_values = (2 * sketch_signs - 1).astype(jnp.float32)
    signed = new_basis * sign_values[None, :]
    sketch = jnp.zeros((columns, SKETCH), jnp.float32).at[:, sketch_rows].add(signed) * math.sqrt(SKETCH / points)
    arnoldi = jnp.stack([projection, spread])
    return (new_basis, sketch, arnoldi)
```

```python
import functools
import math

import jax
import jax.numpy as jnp
from jax import lax
from jax.experimental import pallas as pl
from jax.experimental.pallas import tpu as pltpu
from jax.sharding import PartitionSpec as P

RANK = 16
WIDTH = 32
LEAF = 32
SKETCH = 2048
BOX = "box"


modulus = 8191
epsilon = 1e-06


def swapped(x, axis, bit):
    return lax.ppermute(x, axis, [(i, i ^ 1 << bit) for i in range(lax.axis_size(axis))])


def one_axis_at_a_time(x, axes):
    return lax.psum(x, axes)


def all_sum_kernel(devices, x_ref, o_ref, parts, chunk, gathered, send_sem, recv_sem, gather_send, gather_recv):
    me = lax.axis_index(BOX)
    peers = devices - 1
    barrier = pltpu.get_barrier_semaphore()

    def peer(step):
        return lax.rem(me + step + 1, devices)

    def greet(step, carry):
        pl.semaphore_signal(barrier, inc=1, device_id=(peer(step),), device_id_type=pl.DeviceIdType.MESH)
        return carry

    lax.fori_loop(0, peers, greet, 0)
    pl.semaphore_wait(barrier, peers)

    def scatter(step, carry):
        to = peer(step)
        pltpu.make_async_remote_copy(
            src_ref=x_ref.at[pl.ds(to, 1)],
            dst_ref=parts.at[pl.ds(me, 1)],
            send_sem=send_sem,
            recv_sem=recv_sem,
            device_id=(to,),
            device_id_type=pl.DeviceIdType.MESH,
        ).start()
        return carry

    lax.fori_loop(0, peers, scatter, 0)
    parts[pl.ds(me, 1)] = x_ref[pl.ds(me, 1)]
    pltpu.make_async_copy(parts.at[pl.ds(0, peers)], parts.at[pl.ds(0, peers)], recv_sem).wait()
    chunk[...] = jnp.sum(parts[...], axis=0, keepdims=True)

    def gather(step, carry):
        to = peer(step)
        pltpu.make_async_remote_copy(
            src_ref=chunk,
            dst_ref=gathered.at[pl.ds(me, 1)],
            send_sem=gather_send,
            recv_sem=gather_recv,
            device_id=(to,),
            device_id_type=pl.DeviceIdType.MESH,
        ).start()
        return carry

    lax.fori_loop(0, peers, gather, 0)
    gathered[pl.ds(me, 1)] = chunk[...]
    for done in (gather_recv, gather_send, send_sem):
        pltpu.make_async_copy(gathered.at[pl.ds(0, peers)], gathered.at[pl.ds(0, peers)], done).wait()
    o_ref[...] = gathered[...]


def all_sum(x, devices):
    rows = x.shape[0] * x.shape[1] // devices
    flat = x.reshape(devices, rows)
    call = pl.pallas_call(
        functools.partial(all_sum_kernel, devices),
        out_shape=jax.ShapeDtypeStruct(flat.shape, jnp.float32),
        in_specs=[pl.BlockSpec(memory_space=pltpu.VMEM)],
        out_specs=pl.BlockSpec(memory_space=pltpu.VMEM),
        scratch_shapes=[
            pltpu.VMEM(flat.shape, jnp.float32),
            pltpu.VMEM((1, rows), jnp.float32),
            pltpu.VMEM(flat.shape, jnp.float32),
            pltpu.SemaphoreType.DMA,
            pltpu.SemaphoreType.DMA,
            pltpu.SemaphoreType.DMA,
            pltpu.SemaphoreType.DMA,
        ],
        compiler_params=pltpu.CompilerParams(collective_id=1, has_side_effects=True),
    )
    return call(flat).reshape(x.shape)


def leaf_table(coords, phase_scale):
    scale_mod = phase_scale[0] % modulus
    freq = jnp.arange(RANK, dtype=jnp.int32)
    freq_first = freq % 4 + 1
    freq_second = freq // 4 + 1
    linear = (
        freq_first[:, None] * coords[0][None, :] + freq_second[:, None] * coords[1][None, :]
    ) % modulus
    phase = scale_mod * linear % modulus
    angle = phase.astype(jnp.float32) * (2.0 * math.pi / modulus)
    return jnp.concatenate([jnp.cos(angle), jnp.sin(angle)], 0) * (1.0 / math.sqrt(LEAF))


def translations(box_ids, segment_num, phase_scale):
    scale_mod = phase_scale[0] % modulus
    base_key = (box_ids * 37 + 101 * segment_num) % (modulus - 1) + 1
    unit_phase = scale_mod * base_key % modulus
    indices = jnp.arange(WIDTH, dtype=jnp.int32)
    prod_a = (indices[:, None] + 1) * (indices[None, :] + 2) % modulus
    prod_b = (indices[:, None] + 3) * (indices[None, :] + 1) % modulus
    phase_a = prod_a[:, :, None] * unit_phase[None, None, :] % modulus
    phase_b = (prod_b[:, :, None] * unit_phase[None, None, :] + 4096) % modulus
    factor = 2.0 * math.pi / modulus
    ident = jnp.eye(WIDTH, dtype=jnp.float32)[:, :, None]
    own_map = 0.85 * ident + 0.35 / math.sqrt(WIDTH) * jnp.cos(phase_a.astype(jnp.float32) * factor)
    cross_map = 0.6 / math.sqrt(WIDTH) * jnp.cos(phase_b.astype(jnp.float32) * factor)
    return (own_map, cross_map)


def mix(matrix, coeffs):
    return jnp.einsum("wvg,vgq->wgq", matrix, coeffs, precision=lax.Precision.HIGHEST)


def one_segment(coeffs, segment_num, group_boxes, phase_scale):
    own_map, cross_map = translations(group_boxes, segment_num, phase_scale)
    partner = swapped(coeffs, BOX, segment_num)
    return mix(own_map, coeffs) + mix(cross_map, partner)


def body(basis_vector, diagonal, coords, phase_scale, sketch_rows, sketch_signs):
    highest = lax.Precision.HIGHEST
    columns, local_points = basis_vector.shape
    box_count = local_points // LEAF
    devices = lax.axis_size(BOX)
    segment_count = devices.bit_length() - 1
    rank_id = lax.axis_index(BOX)
    local_ids = jnp.arange(box_count, dtype=jnp.int32)
    group_boxes = rank_id * box_count + local_ids
    leaf_map = leaf_table(coords, phase_scale)
    leaf_boxes = leaf_map.reshape(WIDTH, box_count, LEAF)
    blocks = basis_vector.reshape(columns, box_count, LEAF)
    coeffs = jnp.einsum("wgs,qgs->wgq", leaf_boxes, blocks, precision=highest)
    for segment_num in range(segment_count):
        coeffs = one_segment(coeffs, segment_num, group_boxes, phase_scale)
    applied = jnp.einsum("wgs,wgq->qgs", leaf_boxes, coeffs, precision=highest).reshape(
        columns, local_points
    )
    image = diagonal[None, :] * basis_vector + applied
    total_points = local_points * devices
    sketch_factor = math.sqrt(SKETCH / total_points)
    sign_values = (2 * sketch_signs - 1).astype(jnp.float32)
    block_rows = math.gcd(local_points, 512)
    block_count = local_points // block_rows
    row_blocks = sketch_rows.reshape(block_count, block_rows)
    sketch_ids = jnp.arange(SKETCH, dtype=jnp.int32)
    inner_sum, square_sum = (
        one_axis_at_a_time(jnp.sum(basis_vector * image, axis=1), BOX),
        one_axis_at_a_time(jnp.sum(basis_vector * basis_vector, axis=1), BOX),
    )
    projection = inner_sum / total_points / (square_sum / total_points + epsilon)
    residual = image - projection[:, None] * basis_vector
    energy_sum = one_axis_at_a_time(jnp.sum(residual * residual, axis=1), BOX)
    spread = jnp.sqrt(energy_sum / total_points + epsilon)
    new_basis = residual / spread[:, None]
    signed = (new_basis * sign_values[None, :]).reshape(columns, block_count, block_rows)
    signed = jnp.transpose(signed, (1, 0, 2))

    def add_block(total, pieces):
        piece, rows_here = pieces
        onehot = (rows_here[:, None] == sketch_ids[None, :]).astype(jnp.float32)
        return (
            total + jnp.dot(piece, onehot, precision=highest, preferred_element_type=jnp.float32),
            None,
        )

    total, unused = lax.scan(
        add_block, jnp.zeros((columns, SKETCH), jnp.float32), (signed, row_blocks)
    )
    sketch = all_sum(total, devices) * sketch_factor
    arnoldi = jnp.stack([projection, spread])
    return (new_basis, sketch, arnoldi)


def solution(mesh):
    placed = (P(None, BOX), P(BOX), P(None, BOX), P(), P(BOX), P(BOX))
    return jax.shard_map(
        body, mesh=mesh, in_specs=placed, out_specs=(P(None, BOX), P(), P()), check_vma=False
    )
```

```python
import functools
import math

import jax
import jax.numpy as jnp
from jax import lax
from jax.experimental import pallas as pl
from jax.experimental.pallas import tpu as pltpu
from jax.sharding import PartitionSpec as P

AXIS = "box"
DEVICES = 256
CHIPS = 128
CORES = 2
WIDTH = 32
RANK = 16
LEAF = 32
COLUMNS = 16
SKETCH = 2048
SECTIONS = 8
BOXES = 128
LANES = 128
POINTS = BOXES * LEAF
CHUNKS = POINTS // LANES
TOTAL = POINTS * DEVICES
MODULUS = 8191
EPSILON = 1e-06
SLOT = 8
SENT = 6
BACK = 5
LOW = 256
HIGH = SKETCH // LOW
PIECES = 3
STATE = COLUMNS * WIDTH
MESH = pl.DeviceIdType.MESH

SINE = (3.141592580044348, -5.1677068789061815, 2.550031376988974, -0.5980451725653999, 0.07722012618330765)
COSINE = (
    0.9999999997799037,
    -4.9348021370788295,
    4.058709159556463,
    -1.3352120030521555,
    0.23493731382438812,
    -0.024396324364030414,
)


def fold(x):
    x = (x & MODULUS) + (x >> 13)
    return (x & MODULUS) + (x >> 13)


def turns(phase):
    return (phase << 19) + (phase << 6) + (phase >> 7)


def poly(coefs, y):
    total = jnp.float32(coefs[-1])
    for coef in coefs[-2::-1]:
        total = total * y + jnp.float32(coef)
    return total


def cosine(turn, amplitude):
    r = turn.astype(jnp.float32) * jnp.float32(2.0**-32)
    s = r * poly(SINE, r * r)
    return amplitude - (2.0 * amplitude) * (s * s)


def both(turn, amplitude):
    r = turn.astype(jnp.float32) * jnp.float32(2.0**-32)
    y = r * r
    s = r * poly(SINE, y)
    c = poly(COSINE, y)
    return amplitude - (2.0 * amplitude) * (s * s), (2.0 * amplitude) * (s * c)


def swap_groups(parts):
    parts = list(parts)
    lane = lax.broadcasted_iota(jnp.int32, parts[0].shape, 1)
    for bit in (1, 2):
        shift = 32 * bit
        low = (lane & shift) == 0
        for i in range(4):
            if i & bit:
                continue
            a, b = parts[i], parts[i | bit]
            parts[i] = jnp.where(low, a, pltpu.roll(b, shift, 1))
            parts[i | bit] = jnp.where(low, pltpu.roll(a, LANES - shift, 1), b)
    return parts


def to_lanes(column, offset):
    rows = column.shape[0]
    shape = (rows, LANES)
    here = lax.broadcasted_iota(jnp.int32, shape, 1) == lax.broadcasted_iota(jnp.int32, shape, 0) + offset
    return jnp.sum(jnp.where(here, jnp.broadcast_to(column, shape), 0.0), axis=0, keepdims=True)


def to_column(row, offset, rows):
    shape = (rows, LANES)
    here = lax.broadcasted_iota(jnp.int32, shape, 1) == lax.broadcasted_iota(jnp.int32, shape, 0) + offset
    return jnp.sum(jnp.where(here, jnp.broadcast_to(row, shape), 0.0), axis=1, keepdims=True)


def combine(out_ref, terms, add=False):
    group = 4

    def one_group(g, carry):
        first = pl.multiple_of(g * group * WIDTH, group * WIDTH)
        if add:
            acc = [out_ref[pl.ds(first + 8 * i, 8), :] for i in range(4 * group)]
        else:
            acc = [jnp.zeros((8, LANES), jnp.float32) for _ in range(4 * group)]

        def step(v, acc):
            acc = list(acc)
            for m_ref, base, c_ref in terms:
                rows = [m_ref[pl.ds(pl.multiple_of(base + v * WIDTH, WIDTH) + 8 * t, 8), :] for t in range(4)]
                for i in range(group):
                    c = c_ref[pl.ds(first + i * WIDTH + v, 8, stride=0), :]
                    for t in range(4):
                        acc[4 * i + t] = acc[4 * i + t] + rows[t] * c
            return tuple(acc)

        acc = lax.fori_loop(0, WIDTH, step, tuple(acc), unroll=4)
        for i in range(4 * group):
            out_ref[pl.ds(first + 8 * i, 8), :] = acc[i]
        return carry

    lax.fori_loop(0, COLUMNS // group, one_group, 0)


def build_onehot(onehot_ref, rows_ref):
    def one(c, carry):
        low = jnp.broadcast_to(rows_ref[pl.ds(c, 1), :] & (LOW - 1), (LOW, LANES))
        hit = low == lax.broadcasted_iota(jnp.int32, (LOW, LANES), 0)
        onehot_ref[:, pl.ds(pl.multiple_of(c * LANES, LANES), LANES)] = jnp.where(hit, 1.0, 0.0).astype(jnp.bfloat16)
        return carry

    lax.fori_loop(0, CHUNKS, one, 0, unroll=2)


def scatter_sum(sums_ref, left_ref, onehot_ref, rows_ref, signs_ref, values, acc_ref):
    def one(c, carry):
        x = values(c) * jnp.broadcast_to(signs_ref[pl.ds(c, 1), :], (COLUMNS, LANES))
        high = jnp.broadcast_to(rows_ref[pl.ds(c, 1), :] >> 8, (COLUMNS, LANES))
        here = pl.ds(pl.multiple_of(c * LANES, LANES), LANES)
        pieces = []
        for _ in range(PIECES):
            piece = x.astype(jnp.bfloat16)
            x = x - piece.astype(jnp.float32)
            pieces.append(piece)
        for h in range(HIGH):
            mask = jnp.where(high == h, 1.0, 0.0).astype(jnp.bfloat16)
            for i, piece in enumerate(pieces):
                left_ref[pl.ds((i * HIGH + h) * COLUMNS, COLUMNS), here] = piece * mask
        return carry

    lax.fori_loop(0, CHUNKS, one, 0, unroll=2)
    depth = 512

    def product(k):
        at = pl.ds(pl.multiple_of(k * depth, depth), depth)
        return lax.dot_general(
            left_ref[:, at], onehot_ref[:, at], (((1,), (1,)), ((), ())), preferred_element_type=jnp.float32
        )

    acc_ref[...] = product(0)

    def more(k, carry):
        acc_ref[...] += product(k)
        return carry

    lax.fori_loop(1, POINTS // depth, more, 0)
    rows = HIGH * COLUMNS
    total = acc_ref[pl.ds(0, rows), :] + acc_ref[pl.ds(rows, rows), :] + acc_ref[pl.ds(2 * rows, rows), :]
    for h in range(HIGH):
        for half in range(LOW // LANES):
            block = total[h * COLUMNS : (h + 1) * COLUMNS, half * LANES : (half + 1) * LANES]
            sums_ref[pl.ds(h * (LOW // LANES) + half, COLUMNS, stride=SKETCH // LANES), :] = block


def make_sections(matrix_ref, scale, group, chip):
    own_size = 0.35 / math.sqrt(WIDTH)
    cross_size = 0.6 / math.sqrt(WIDTH)
    sub = lax.broadcasted_iota(jnp.int32, (8, LANES), 0)
    box = group * BOXES + chip

    def one(k, carry):
        key = box * 37 + 101 * k
        guess = (key.astype(jnp.float32) * jnp.float32(1.0 / (MODULUS - 1))).astype(jnp.int32)
        key = key - guess * (MODULUS - 1)
        key = jnp.where(key < 0, key + (MODULUS - 1), key)
        key = jnp.where(key >= MODULUS - 1, key - (MODULUS - 1), key)
        unit = fold(scale * (key + 1))
        base = pl.multiple_of(k * (2 * WIDTH * WIDTH), 2 * WIDTH * WIDTH)
        half = turns(jnp.int32(4096))
        for t in range(4):
            own_step = turns(fold((sub + (8 * t + 1)) * unit))
            cross_step = turns(fold((sub + (8 * t + 3)) * unit))
            own_turn = own_step
            cross_turn = jnp.broadcast_to(half, (8, LANES))
            for v in range(WIDTH):
                own_turn = own_turn + own_step
                cross_turn = cross_turn + cross_step
                own = cosine(own_turn, own_size)
                if v // 8 == t:
                    own = own + jnp.where(sub == v % 8, 0.85, 0.0)
                matrix_ref[pl.ds(base + v * WIDTH + 8 * t, 8), :] = own
                matrix_ref[pl.ds(base + WIDTH * WIDTH + v * WIDTH + 8 * t, 8), :] = cosine(cross_turn, cross_size)
        return carry

    return one


def kernel(
    basis_ref, diag_ref, coords_ref, scale_ref, rows_ref, signs_ref,
    new_ref, sketch_ref, arnoldi_ref,
    tall, pack, flat_x, out_box, in_box, matrix, leaf, leaf_t, state_x,
    first, second, first_p, partner, point, point_rows, residual,
    out_back, in_back, onehot, left, acc, sums_b, parts_b, row_b, all_b, sums_r, parts_r, row_r, all_r,
    half_mine, half_other, shift_rows, signs_f,
    fwd_s, fwd_r, ex_s, ex_r, rsb_s, rsb_r, agb_s, agb_r, rs_s, rs_r, ag_s, ag_r, back_s, back_r, mom_s, mom_r,
):
    me = lax.axis_index(AXIS)
    chip = me // CORES
    core = lax.rem(me, CORES)
    other = me + 1 - 2 * core
    barrier = pltpu.get_barrier_semaphore()
    peers = DEVICES - 1
    mates = CHIPS - 1

    def peer(step):
        return lax.rem(me + step + 1, DEVICES)

    def mate(step):
        return lax.rem(me + CORES * (step + 1), DEVICES)

    def each(count, what, unroll=1):
        def body(step, carry):
            what(step)
            return carry

        lax.fori_loop(0, count, body, 0, unroll=unroll)

    def remote(src, dst, send, recv, to):
        return pltpu.make_async_remote_copy(
            src_ref=src, dst_ref=dst, send_sem=send, recv_sem=recv, device_id=(to,), device_id_type=MESH
        )

    def settle(ref, rows, sem):
        pltpu.make_async_copy(ref.at[pl.ds(0, rows)], ref.at[pl.ds(0, rows)], sem).wait()

    each(peers, lambda i: pl.semaphore_signal(barrier, inc=1, device_id=(peer(i),), device_id_type=MESH))

    square = jnp.zeros((COLUMNS, LANES), jnp.float32)
    weighted = jnp.zeros((COLUMNS, LANES), jnp.float32)
    for c in range(CHUNKS):
        x = basis_ref[:, c * LANES : (c + 1) * LANES]
        tall[pl.ds(c * COLUMNS, COLUMNS), :] = x
        pack[pl.ds(2 * c, 2), :] = coords_ref[:, c * LANES : (c + 1) * LANES].astype(jnp.float32)
        d = jnp.broadcast_to(diag_ref[pl.ds(c, 1), :], (COLUMNS, LANES))
        square = square + x * x
        weighted = weighted + d * x * x
    moments = to_lanes(jnp.sum(square, axis=1, keepdims=True), 32) + to_lanes(
        jnp.sum(weighted, axis=1, keepdims=True), 48
    )
    sign = (2 * signs_ref[...] - 1).astype(jnp.float32)
    signs_f[...] = sign
    for rho in range(4):
        blocks = swap_groups([tall[pl.ds(4 * rho + t, CHUNKS, stride=COLUMNS), :] for t in range(4)])
        for j in range(4):
            out_box[pl.ds(SLOT * j + rho, CHUNKS, stride=4 * SLOT), :] = blocks[j]
    blocks = swap_groups(
        [
            pack[pl.ds(0, CHUNKS, stride=2), :],
            pack[pl.ds(1, CHUNKS, stride=2), :],
            diag_ref[...],
            rows_ref[...].astype(jnp.float32),
        ]
    )
    for j in range(4):
        out_box[pl.ds(SLOT * j + 4, CHUNKS, stride=4 * SLOT), :] = blocks[j]
    zero = jnp.zeros((CHUNKS, LANES), jnp.float32)
    blocks = swap_groups([sign, zero, zero, zero])
    for j in range(4):
        out_box[pl.ds(SLOT * j + 5, CHUNKS, stride=4 * SLOT), :] = blocks[j] + moments

    scale = lax.rem(scale_ref[0], MODULUS)
    group = lax.broadcasted_iota(jnp.int32, (8, LANES), 1) * CORES + core
    section = make_sections(matrix, scale, group, chip)
    lax.fori_loop(0, 4, section, 0)

    pl.semaphore_wait(barrier, peers)

    def send_box(i):
        to = mate(i)
        remote(
            out_box.at[pl.ds(pl.multiple_of(SLOT * (to // CORES), SLOT), SENT)],
            in_box.at[pl.ds(pl.multiple_of(SLOT * chip, SLOT), SENT)],
            fwd_s, fwd_r, to,
        ).start()

    each(mates, send_box)
    mine = pl.ds(pl.multiple_of(SLOT * chip, SLOT), SLOT)
    in_box[mine, :] = out_box[mine, :]
    lax.fori_loop(4, SECTIONS, section, 0)

    build_onehot(onehot, rows_ref)
    scatter_sum(
        sums_b, left, onehot, rows_ref, signs_f,
        lambda c: tall[pl.ds(pl.multiple_of(c * COLUMNS, COLUMNS), COLUMNS), :], acc,
    )

    def spread_rows(src, dst, send, recv):
        def go(i):
            to = peer(i)
            remote(src.at[pl.ds(to, 1)], dst.at[pl.ds(me, 1)], send, recv, to).start()

        each(peers, go)
        dst[pl.ds(me, 1), :] = src[pl.ds(me, 1), :]

    def gather_rows(row, dst, send, recv):
        def go(i):
            remote(row, dst.at[pl.ds(me, 1)], send, recv, peer(i)).start()

        each(peers, go)
        dst[pl.ds(me, 1), :] = row[...]

    spread_rows(sums_b, parts_b, rsb_s, rsb_r)

    settle(in_box, mates * SENT, fwd_r)
    for rho in range(4):
        state_x[pl.ds(rho * LANES, LANES), :] = in_box[pl.ds(rho, CHIPS, stride=SLOT), :].T
    point[...] = in_box[pl.ds(4, CHIPS, stride=SLOT), :].T
    tail = in_box[pl.ds(5, CHIPS, stride=SLOT), :].T
    signs_f[...] = tail[0:LEAF, :]
    point_rows[...] = point[pl.ds(3 * LEAF, LEAF), :].astype(jnp.int32)
    first[pl.ds(STATE, 2 * COLUMNS), :] = jnp.broadcast_to(
        jnp.sum(tail[LEAF : LEAF + 2 * COLUMNS, :], axis=1, keepdims=True), (2 * COLUMNS, LANES)
    )

    size = 1.0 / math.sqrt(LEAF)
    across = point[pl.ds(0, LEAF), :].astype(jnp.int32) * scale
    down = point[pl.ds(LEAF, LEAF), :].astype(jnp.int32) * scale
    turn_x = [turns(fold(across * f)) for f in range(1, 5)]
    turn_y = [turns(fold(down * f)) for f in range(1, 5)]
    for w in range(RANK):
        c, s = both(turn_x[w % 4] + turn_y[w // 4], size)
        for at, table in ((w, c), (w + RANK, s)):
            leaf[pl.ds(at * LEAF, LEAF), :] = table
            leaf_t[pl.ds(at, LEAF, stride=WIDTH), :] = table
    combine(first, [(leaf_t, 0, state_x)])

    exchange = remote(first, first_p, ex_s, ex_r, other)
    exchange.start()
    combine(second, [(matrix, 0, first)])
    build_onehot(onehot, point_rows)
    exchange.wait_recv()
    combine(second, [(matrix, WIDTH * WIDTH, first_p)], add=True)
    exchange.wait_send()

    source, target = second, first
    for k in range(1, SECTIONS):
        step = 1 << (k - 1)

        def swap(r, source=source, step=step):
            at = pl.ds(pl.multiple_of(r * 64, 64), 64)
            a = source[at, :]
            up = (lax.broadcasted_iota(jnp.int32, a.shape, 1) & step) != 0
            partner[at, :] = jnp.where(up, pltpu.roll(a, step, 1), pltpu.roll(a, LANES - step, 1))

        each(STATE // 64, swap)
        base = k * 2 * WIDTH * WIDTH
        combine(target, [(matrix, base, source), (matrix, base + WIDTH * WIDTH, partner)])
        source, target = target, source
        if k == 2:
            settle(parts_b, peers, rsb_r)
            row_b[...] = jnp.sum(parts_b[...], axis=0, keepdims=True)
            gather_rows(row_b, all_b, agb_s, agb_r)

    both_sums = first_p[pl.ds(STATE, 2 * COLUMNS), :] + half_mine_sum(first)
    total_b = both_sums[0:COLUMNS, :]
    total_db = both_sums[COLUMNS:, :]
    weight = total_b + EPSILON * TOTAL
    shift_rows[...] = total_db / weight
    combine(residual, [(leaf, 0, source)])
    cross_sum = []
    square_sum = []
    for q in range(COLUMNS):
        p0 = jnp.broadcast_to(shift_rows[pl.ds(q, 1), :], (LEAF, LANES))
        b = state_x[pl.ds(q * LEAF, LEAF), :]
        r = (point[pl.ds(2 * LEAF, LEAF), :] - p0) * b + residual[pl.ds(q * LEAF, LEAF), :]
        residual[pl.ds(q * LEAF, LEAF), :] = r
        cross_sum.append(jnp.sum(b * r, axis=0, keepdims=True))
        square_sum.append(jnp.sum(r * r, axis=0, keepdims=True))
    moments = jnp.sum(jnp.concatenate(cross_sum + square_sum, axis=0), axis=1, keepdims=True)
    scatter_sum(
        sums_r, left, onehot, point_rows, signs_f,
        lambda c: residual[pl.ds(c, COLUMNS, stride=LEAF), :], acc,
    )
    spread_rows(sums_r, parts_r, rs_s, rs_r)

    for rho in range(4):
        out_back[pl.ds(rho, CHIPS, stride=SLOT), :] = residual[pl.ds(rho * LANES, LANES), :].T
    out_back[pl.ds(4, CHIPS, stride=SLOT), :] = jnp.broadcast_to(to_lanes(moments, 0), (CHIPS, LANES))

    def send_back(i):
        to = mate(i)
        remote(
            out_back.at[pl.ds(pl.multiple_of(SLOT * (to // CORES), SLOT), BACK)],
            in_back.at[pl.ds(pl.multiple_of(SLOT * chip, SLOT), BACK)],
            back_s, back_r, to,
        ).start()

    each(mates, send_back)
    in_back[mine, :] = out_back[mine, :]

    settle(parts_r, peers, rs_r)
    row_r[...] = jnp.sum(parts_r[...], axis=0, keepdims=True)
    gather_rows(row_r, all_r, ag_s, ag_r)

    settle(in_back, mates * BACK, back_r)
    half_mine[...] = jnp.broadcast_to(
        jnp.sum(in_back[pl.ds(4, CHIPS, stride=SLOT), :], axis=0, keepdims=True), (8, LANES)
    )
    swap_sums = remote(half_mine, half_other, mom_s, mom_r, other)
    swap_sums.start()
    for rho in range(4):
        blocks = swap_groups([in_back[pl.ds(SLOT * j + rho, CHUNKS, stride=4 * SLOT), :] for j in range(4)])
        for t in range(4):
            flat_x[pl.ds(4 * rho + t, CHUNKS, stride=COLUMNS), :] = blocks[t]
    swap_sums.wait()
    sums = to_column(half_mine[0:1, :] + half_other[0:1, :], 0, 2 * COLUMNS)
    sums = jnp.broadcast_to(sums, (2 * COLUMNS, LANES))
    m1 = sums[0:COLUMNS, :]
    m2 = sums[COLUMNS:, :]
    p0 = shift_rows[...]
    delta = (m1 - p0 * (EPSILON * TOTAL)) / weight
    energy = m2 - 2.0 * delta * m1 + delta * delta * total_b
    spread = jnp.sqrt(jnp.maximum(energy, 0.0) * (1.0 / TOTAL) + EPSILON)
    inverse = 1.0 / spread
    arnoldi_ref[0:1, :] = to_lanes((p0 + delta)[:, 0:1], 0)[:, 0:COLUMNS]
    arnoldi_ref[1:2, :] = to_lanes(spread[:, 0:1], 0)[:, 0:COLUMNS]
    for c in range(CHUNKS):
        at = pl.ds(c * COLUMNS, COLUMNS)
        new_ref[:, c * LANES : (c + 1) * LANES] = (flat_x[at, :] - delta * tall[at, :]) * inverse

    settle(all_b, peers, agb_r)
    settle(all_r, peers, ag_r)
    factor = inverse * math.sqrt(SKETCH / TOTAL)
    for r in range(SKETCH // LANES):
        at = pl.ds(r, COLUMNS, stride=SKETCH // LANES)
        sketch_ref[:, r * LANES : (r + 1) * LANES] = (all_r[at, :] - delta * all_b[at, :]) * factor

    settle(out_box, mates * SENT, fwd_s)
    settle(sums_b, peers, rsb_s)
    settle(all_b, peers, agb_s)
    settle(sums_r, peers, rs_s)
    settle(all_r, peers, ag_s)
    settle(out_back, mates * BACK, back_s)


def half_mine_sum(first):
    return first[pl.ds(STATE, 2 * COLUMNS), :]


def body(basis_vector, diagonal, coords, phase_scale, sketch_rows, sketch_signs):
    f32 = jnp.float32
    vmem = pl.BlockSpec(memory_space=pltpu.VMEM)
    box_rows = CHIPS * SLOT
    scratch = [
        pltpu.VMEM((CHUNKS * COLUMNS, LANES), f32),
        pltpu.VMEM((2 * CHUNKS, LANES), f32),
        pltpu.VMEM((CHUNKS * COLUMNS, LANES), f32),
        pltpu.VMEM((box_rows, LANES), f32),
        pltpu.VMEM((box_rows, LANES), f32),
        pltpu.VMEM((SECTIONS * 2 * WIDTH * WIDTH, LANES), f32),
        pltpu.VMEM((WIDTH * LEAF, LANES), f32),
        pltpu.VMEM((WIDTH * LEAF, LANES), f32),
        pltpu.VMEM((STATE, LANES), f32),
        pltpu.VMEM((STATE + 2 * COLUMNS, LANES), f32),
        pltpu.VMEM((STATE, LANES), f32),
        pltpu.VMEM((STATE + 2 * COLUMNS, LANES), f32),
        pltpu.VMEM((STATE, LANES), f32),
        pltpu.VMEM((4 * LEAF, LANES), f32),
        pltpu.VMEM((LEAF, LANES), jnp.int32),
        pltpu.VMEM((STATE, LANES), f32),
        pltpu.VMEM((box_rows, LANES), f32),
        pltpu.VMEM((box_rows, LANES), f32),
        pltpu.VMEM((LOW, POINTS), jnp.bfloat16),
        pltpu.VMEM((PIECES * HIGH * COLUMNS, POINTS), jnp.bfloat16),
        pltpu.VMEM((PIECES * HIGH * COLUMNS, LOW), f32),
    ]
    for _ in range(2):
        scratch += [
            pltpu.VMEM((DEVICES, LANES), f32),
            pltpu.VMEM((DEVICES, LANES), f32),
            pltpu.VMEM((1, LANES), f32),
            pltpu.VMEM((DEVICES, LANES), f32),
        ]
    scratch += [
        pltpu.VMEM((8, LANES), f32),
        pltpu.VMEM((8, LANES), f32),
        pltpu.VMEM((COLUMNS, LANES), f32),
        pltpu.VMEM((LEAF, LANES), f32),
    ]
    scratch += [pltpu.SemaphoreType.DMA] * 16
    call = pl.pallas_call(
        kernel,
        out_shape=(
            jax.ShapeDtypeStruct((COLUMNS, POINTS), f32),
            jax.ShapeDtypeStruct((COLUMNS, SKETCH), f32),
            jax.ShapeDtypeStruct((2, COLUMNS), f32),
        ),
        in_specs=[vmem, vmem, vmem, pl.BlockSpec(memory_space=pltpu.SMEM), vmem, vmem],
        out_specs=(vmem, vmem, vmem),
        scratch_shapes=scratch,
        compiler_params=pltpu.CompilerParams(collective_id=1, has_side_effects=True, vmem_limit_bytes=48 << 20),
    )
    table = (CHUNKS, LANES)
    return call(
        basis_vector,
        diagonal.reshape(table),
        coords,
        phase_scale,
        sketch_rows.reshape(table),
        sketch_signs.reshape(table),
    )


def solution(mesh):
    placed = (P(None, AXIS), P(AXIS), P(None, AXIS), P(), P(AXIS), P(AXIS))
    return jax.shard_map(
        body, mesh=mesh, in_specs=placed, out_specs=(P(None, AXIS), P(), P()), check_vma=False
    )
```

```python
import functools
import math

import jax
import jax.numpy as jnp
from jax import lax
from jax.experimental import pallas as pl
from jax.experimental.pallas import tpu as pltpu
from jax.sharding import PartitionSpec as P

AXIS = "box"
DEVICES = 256
CHIPS = 128
CORES = 2
WIDTH = 32
RANK = 16
LEAF = 32
COLUMNS = 16
SKETCH = 2048
SECTIONS = 8
BOXES = 128
LANES = 128
POINTS = BOXES * LEAF
CHUNKS = POINTS // LANES
TOTAL = POINTS * DEVICES
MODULUS = 8191
EPSILON = 1e-06
SLOT = 8
SENT = 6
BACK = 5
LOW = 256
HIGH = SKETCH // LOW
PIECES = 2
STATE = COLUMNS * WIDTH
MESH = pl.DeviceIdType.MESH

SINE = (3.141592580044348, -5.1677068789061815, 2.550031376988974, -0.5980451725653999, 0.07722012618330765)
COSINE = (
    0.9999999997799037,
    -4.9348021370788295,
    4.058709159556463,
    -1.3352120030521555,
    0.23493731382438812,
    -0.024396324364030414,
)


def fold(x):
    x = (x & MODULUS) + (x >> 13)
    return (x & MODULUS) + (x >> 13)


def turns(phase):
    return (phase << 19) + (phase << 6) + (phase >> 7)


def poly(coefs, y):
    total = jnp.float32(coefs[-1])
    for coef in coefs[-2::-1]:
        total = total * y + jnp.float32(coef)
    return total


def cosine(turn, amplitude):
    r = turn.astype(jnp.float32) * jnp.float32(2.0**-32)
    s = r * poly(SINE, r * r)
    return amplitude - (2.0 * amplitude) * (s * s)


def both(turn, amplitude):
    r = turn.astype(jnp.float32) * jnp.float32(2.0**-32)
    y = r * r
    s = r * poly(SINE, y)
    c = poly(COSINE, y)
    return amplitude - (2.0 * amplitude) * (s * s), (2.0 * amplitude) * (s * c)


def swap_groups(parts):
    parts = list(parts)
    lane = lax.broadcasted_iota(jnp.int32, parts[0].shape, 1)
    for bit in (1, 2):
        shift = 32 * bit
        low = (lane & shift) == 0
        for i in range(4):
            if i & bit:
                continue
            a, b = parts[i], parts[i | bit]
            parts[i] = jnp.where(low, a, pltpu.roll(b, shift, 1))
            parts[i | bit] = jnp.where(low, pltpu.roll(a, LANES - shift, 1), b)
    return parts


def to_lanes(column, offset):
    rows = column.shape[0]
    shape = (rows, LANES)
    here = lax.broadcasted_iota(jnp.int32, shape, 1) == lax.broadcasted_iota(jnp.int32, shape, 0) + offset
    return jnp.sum(jnp.where(here, jnp.broadcast_to(column, shape), 0.0), axis=0, keepdims=True)


def to_column(row, offset, rows):
    shape = (rows, LANES)
    here = lax.broadcasted_iota(jnp.int32, shape, 1) == lax.broadcasted_iota(jnp.int32, shape, 0) + offset
    return jnp.sum(jnp.where(here, jnp.broadcast_to(row, shape), 0.0), axis=1, keepdims=True)


def combine(out_ref, terms, add=False):
    group = 4

    def one_group(g, carry):
        first = pl.multiple_of(g * group * WIDTH, group * WIDTH)
        if add:
            acc = [out_ref[pl.ds(first + 8 * i, 8), :] for i in range(4 * group)]
        else:
            acc = [jnp.zeros((8, LANES), jnp.float32) for _ in range(4 * group)]

        def step(v, acc):
            acc = list(acc)
            for m_ref, base, c_ref in terms:
                rows = [m_ref[pl.ds(pl.multiple_of(base + v * WIDTH, WIDTH) + 8 * t, 8), :] for t in range(4)]
                for i in range(group):
                    c = c_ref[pl.ds(first + i * WIDTH + v, 8, stride=0), :]
                    for t in range(4):
                        acc[4 * i + t] = acc[4 * i + t] + rows[t] * c
            return tuple(acc)

        acc = lax.fori_loop(0, WIDTH, step, tuple(acc), unroll=8)
        for i in range(4 * group):
            out_ref[pl.ds(first + 8 * i, 8), :] = acc[i]
        return carry

    lax.fori_loop(0, COLUMNS // group, one_group, 0)


def build_onehot(onehot_ref, rows_ref):
    def one(c, carry):
        low = (rows_ref[pl.ds(c, 1), :] & (LOW - 1)).astype(jnp.float32)
        low = jnp.broadcast_to(low, (16, LANES)).astype(jnp.bfloat16)
        sub = lax.broadcasted_iota(jnp.int32, (16, LANES), 0).astype(jnp.float32)
        one_b = jnp.ones((16, LANES), jnp.bfloat16)
        zero_b = jnp.zeros((16, LANES), jnp.bfloat16)
        here = pl.ds(pl.multiple_of(c * LANES, LANES), LANES)
        for r in range(LOW // 16):
            hit = low == (sub + float(16 * r)).astype(jnp.bfloat16)
            onehot_ref[pl.ds(16 * r, 16), here] = jnp.where(hit, one_b, zero_b)
        return carry

    lax.fori_loop(0, CHUNKS, one, 0, unroll=2)


def scatter_sum(sums_ref, left_ref, onehot_ref, rows_ref, signs_ref, values, acc_ref):
    def one(c, carry):
        x = values(c) * jnp.broadcast_to(signs_ref[pl.ds(c, 1), :], (COLUMNS, LANES))
        high = (rows_ref[pl.ds(c, 1), :] >> 8).astype(jnp.float32)
        high = jnp.broadcast_to(high, (COLUMNS, LANES)).astype(jnp.bfloat16)
        zero_b = jnp.zeros((COLUMNS, LANES), jnp.bfloat16)
        here = pl.ds(pl.multiple_of(c * LANES, LANES), LANES)
        pieces = []
        for _ in range(PIECES):
            piece = x.astype(jnp.bfloat16)
            x = x - piece.astype(jnp.float32)
            pieces.append(piece)
        for h in range(HIGH):
            hit = high == jnp.full((COLUMNS, LANES), h, jnp.bfloat16)
            for i, piece in enumerate(pieces):
                left_ref[pl.ds((i * HIGH + h) * COLUMNS, COLUMNS), here] = jnp.where(hit, piece, zero_b)
        return carry

    lax.fori_loop(0, CHUNKS, one, 0, unroll=2)
    acc_ref[...] = lax.dot_general(
        left_ref[...], onehot_ref[...], (((1,), (1,)), ((), ())), preferred_element_type=jnp.float32
    )
    rows = HIGH * COLUMNS
    total = acc_ref[pl.ds(0, rows), :] + acc_ref[pl.ds(rows, rows), :]
    for h in range(HIGH):
        for half in range(LOW // LANES):
            block = total[h * COLUMNS : (h + 1) * COLUMNS, half * LANES : (half + 1) * LANES]
            sums_ref[pl.ds(h * (LOW // LANES) + half, COLUMNS, stride=SKETCH // LANES), :] = block


def make_sections(matrix_ref, scale, group, chip):
    own_size = 0.35 / math.sqrt(WIDTH)
    cross_size = 0.6 / math.sqrt(WIDTH)
    sub = lax.broadcasted_iota(jnp.int32, (8, LANES), 0)
    box = group * BOXES + chip

    def one(k, carry):
        key = box * 37 + 101 * k
        guess = (key.astype(jnp.float32) * jnp.float32(1.0 / (MODULUS - 1))).astype(jnp.int32)
        key = key - guess * (MODULUS - 1)
        key = jnp.where(key < 0, key + (MODULUS - 1), key)
        key = jnp.where(key >= MODULUS - 1, key - (MODULUS - 1), key)
        unit = fold(scale * (key + 1))
        base = pl.multiple_of(k * (2 * WIDTH * WIDTH), 2 * WIDTH * WIDTH)
        half = turns(jnp.int32(4096))
        for t in range(4):
            own_step = turns(fold((sub + (8 * t + 1)) * unit))
            cross_step = turns(fold((sub + (8 * t + 3)) * unit))
            own_turn = own_step
            cross_turn = jnp.broadcast_to(half, (8, LANES))
            for v in range(WIDTH):
                own_turn = own_turn + own_step
                cross_turn = cross_turn + cross_step
                own = cosine(own_turn, own_size)
                if v // 8 == t:
                    own = own + jnp.where(sub == v % 8, 0.85, 0.0)
                matrix_ref[pl.ds(base + v * WIDTH + 8 * t, 8), :] = own
                matrix_ref[pl.ds(base + WIDTH * WIDTH + v * WIDTH + 8 * t, 8), :] = cosine(cross_turn, cross_size)
        return carry

    return one


def kernel(
    basis_hbm, diag_hbm, coords_hbm, scale_ref, rows_hbm, signs_hbm,
    new_ref, sketch_ref, arnoldi_ref,
    tall, pack, flat_x, out_box, in_box, matrix, leaf, leaf_t, state_x,
    first, second, first_p, partner, point, point_rows, residual,
    out_c, in_c, half_b, other_b,
    out_back, in_back, onehot, left, acc, sums_b, parts_b, row_b, all_b, sums_r, parts_r, row_r, all_r,
    half_mine, half_other, shift_rows, signs_f,
    basis_ref, diag_ref, coords_ref, rows_ref, signs_ref, load_sem,
    fwd_s, fwd_r, ex_s, ex_r, rsb_s, rsb_r, agb_s, agb_r, rs_s, rs_r, ag_s, ag_r, back_s, back_r, mom_s, mom_r,
    coef_s, coef_r, hb_s, hb_r,
):
    me = lax.axis_index(AXIS)
    chip = me // CORES
    core = lax.rem(me, CORES)
    other = me + 1 - 2 * core
    barrier = pltpu.get_barrier_semaphore()
    peers = DEVICES - 1
    mates = CHIPS - 1

    x = lax.rem(chip, 4)
    z = lax.rem(me // 8, 8)
    y = me // 64
    x_at = [lax.rem(x + i, 4) * 2 for i in range(4)]
    y_at = [lax.rem(y + i, 4) * 64 for i in range(4)]
    core_at = [core, 1 - core]

    def far_first(what, cores):
        steps = [(a, b, c) for a in range(4) for b in range(4) for c in range(cores)]
        steps.sort(key=lambda s: -(min(s[0], 4 - s[0]) + min(s[1], 4 - s[1]) + 0.1 * s[2]))
        near = [[y_at[a] + x_at[b] + core_at[c] for b in range(4)] for a in range(4) for c in range(cores)]

        def layer(dz, own):
            base = lax.rem(z + dz, 8) * 8
            for a, b, c in steps:
                if own and (a, b, c) == (0, 0, 0):
                    continue
                what(near[a * cores + c][b] + base)

        def body(i, carry):
            layer(4 + ((i + 1) // 2) * (1 - 2 * lax.rem(i, 2)), False)
            return carry

        lax.fori_loop(0, 7, body, 0)
        layer(0, True)

    def each(count, what, unroll=1):
        def body(step, carry):
            what(step)
            return carry

        lax.fori_loop(0, count, body, 0, unroll=unroll)

    def remote(src, dst, send, recv, to):
        return pltpu.make_async_remote_copy(
            src_ref=src, dst_ref=dst, send_sem=send, recv_sem=recv, device_id=(to,), device_id_type=MESH
        )

    def settle(ref, rows, sem):
        pltpu.make_async_copy(ref.at[pl.ds(0, rows)], ref.at[pl.ds(0, rows)], sem).wait()

    loads = []
    for i, (src, dst) in enumerate(
        [(basis_hbm, basis_ref), (coords_hbm, coords_ref), (diag_hbm, diag_ref), (rows_hbm, rows_ref), (signs_hbm, signs_ref)]
    ):
        loads.append(pltpu.make_async_copy(src, dst, load_sem.at[i]))
        loads[-1].start()
    far_first(lambda to: pl.semaphore_signal(barrier, inc=1, device_id=(to,), device_id_type=MESH), 2)
    for load in loads:
        load.wait()

    square = jnp.zeros((COLUMNS, LANES), jnp.float32)
    weighted = jnp.zeros((COLUMNS, LANES), jnp.float32)
    for c in range(CHUNKS):
        x = basis_ref[:, c * LANES : (c + 1) * LANES]
        tall[pl.ds(c * COLUMNS, COLUMNS), :] = x
        pack[pl.ds(2 * c, 2), :] = coords_ref[:, c * LANES : (c + 1) * LANES].astype(jnp.float32)
        d = jnp.broadcast_to(diag_ref[pl.ds(c, 1), :], (COLUMNS, LANES))
        square = square + x * x
        weighted = weighted + d * x * x
    moments = to_lanes(jnp.sum(square, axis=1, keepdims=True), 32) + to_lanes(
        jnp.sum(weighted, axis=1, keepdims=True), 48
    )
    sign = (2 * signs_ref[...] - 1).astype(jnp.float32)
    signs_f[...] = sign
    for rho in range(4):
        blocks = swap_groups([tall[pl.ds(4 * rho + t, CHUNKS, stride=COLUMNS), :] for t in range(4)])
        for j in range(4):
            out_box[pl.ds(SLOT * j + rho, CHUNKS, stride=4 * SLOT), :] = blocks[j]
    blocks = swap_groups(
        [
            pack[pl.ds(0, CHUNKS, stride=2), :],
            pack[pl.ds(1, CHUNKS, stride=2), :],
            diag_ref[...],
            rows_ref[...].astype(jnp.float32),
        ]
    )
    for j in range(4):
        out_box[pl.ds(SLOT * j + 4, CHUNKS, stride=4 * SLOT), :] = blocks[j]
    zero = jnp.zeros((CHUNKS, LANES), jnp.float32)
    blocks = swap_groups([sign, zero, zero, zero])
    for j in range(4):
        out_box[pl.ds(SLOT * j + 5, CHUNKS, stride=4 * SLOT), :] = blocks[j] + moments

    scale = lax.rem(scale_ref[0], MODULUS)
    size = 1.0 / math.sqrt(LEAF)

    def leaf_tables(store):
        across = point[pl.ds(0, LEAF), :].astype(jnp.int32) * scale
        down = point[pl.ds(LEAF, LEAF), :].astype(jnp.int32) * scale
        turn_x = [turns(fold(across * f)) for f in range(1, 5)]
        turn_y = [turns(fold(down * f)) for f in range(1, 5)]
        for w in range(RANK):
            c, s = both(turn_x[w % 4] + turn_y[w // 4], size)
            store(w, c)
            store(w + RANK, s)

    def store_by_point(w, table):
        leaf_t[pl.ds(w, LEAF, stride=WIDTH), :] = table

    def store_by_width(w, table):
        leaf[pl.ds(w * LEAF, LEAF), :] = table

    for rho in range(4):
        state_x[pl.ds(rho * LANES, LANES), :] = out_box[pl.ds(rho, CHIPS, stride=SLOT), :].T
    point[...] = out_box[pl.ds(4, CHIPS, stride=SLOT), :].T
    leaf_tables(store_by_point)
    combine(second, [(leaf_t, 0, state_x)])
    for rho in range(4):
        out_c[pl.ds(rho, CHIPS, stride=SLOT), :] = second[pl.ds(rho * LANES, LANES), :].T

    pl.semaphore_wait(barrier, peers)

    def send_slots(src, dst, count, send, recv):
        def go(to):
            remote(
                src.at[pl.ds(pl.multiple_of(SLOT * (to // CORES), SLOT), count)],
                dst.at[pl.ds(pl.multiple_of(SLOT * chip, SLOT), count)],
                send, recv, to,
            ).start()

        far_first(go, 1)
        mine = pl.ds(pl.multiple_of(SLOT * chip, SLOT), count)
        dst[mine, :] = src[mine, :]

    send_slots(out_c, in_c, 4, coef_s, coef_r)

    def spread_rows(src, dst, send, recv):
        def go(to):
            remote(src.at[pl.ds(to, 1)], dst.at[pl.ds(me, 1)], send, recv, to).start()

        far_first(go, 2)
        dst[pl.ds(me, 1), :] = src[pl.ds(me, 1), :]

    def gather_rows(row, dst, send, recv):
        def go(to):
            remote(row, dst.at[pl.ds(me, 1)], send, recv, to).start()

        far_first(go, 2)
        dst[pl.ds(me, 1), :] = row[...]

    build_onehot(onehot, rows_ref)
    scatter_sum(
        sums_b, left, onehot, rows_ref, signs_f,
        lambda c: tall[pl.ds(pl.multiple_of(c * COLUMNS, COLUMNS), COLUMNS), :], acc,
    )
    spread_rows(sums_b, parts_b, rsb_s, rsb_r)
    send_slots(out_box, in_box, SENT, fwd_s, fwd_r)
    group = lax.broadcasted_iota(jnp.int32, (8, LANES), 1) * CORES + core
    lax.fori_loop(0, SECTIONS, make_sections(matrix, scale, group, chip), 0)

    settle(in_c, mates * 4, coef_r)
    for rho in range(4):
        first[pl.ds(rho * LANES, LANES), :] = in_c[pl.ds(rho, CHIPS, stride=SLOT), :].T

    exchange = remote(first, first_p, ex_s, ex_r, other)
    exchange.start()
    combine(second, [(matrix, 0, first)])
    exchange.wait_recv()
    combine(second, [(matrix, WIDTH * WIDTH, first_p)], add=True)
    exchange.wait_send()
    source, target = second, first
    for k in range(1, SECTIONS):
        step = 1 << (k - 1)

        def swap(r, source=source, step=step):
            at = pl.ds(pl.multiple_of(r * 512, 512), 512)
            a = source[at, :]
            up = (lax.broadcasted_iota(jnp.int32, a.shape, 1) & step) != 0
            partner[at, :] = jnp.where(up, pltpu.roll(a, step, 1), pltpu.roll(a, LANES - step, 1))

        each(STATE // 512, swap)
        base = k * 2 * WIDTH * WIDTH
        combine(target, [(matrix, base, source), (matrix, base + WIDTH * WIDTH, partner)])
        source, target = target, source
        if k == 2:
            settle(parts_b, peers, rsb_r)
            row_b[...] = jnp.sum(parts_b[...], axis=0, keepdims=True)
            gather_rows(row_b, all_b, agb_s, agb_r)

    settle(in_box, mates * SENT, fwd_r)
    tail = in_box[pl.ds(5, CHIPS, stride=SLOT), :].T
    half_b[...] = jnp.broadcast_to(
        jnp.sum(tail[LEAF : LEAF + 2 * COLUMNS, :], axis=1, keepdims=True), (2 * COLUMNS, LANES)
    )
    swap_b = remote(half_b, other_b, hb_s, hb_r, other)
    swap_b.start()
    signs_f[...] = tail[0:LEAF, :]
    for rho in range(4):
        state_x[pl.ds(rho * LANES, LANES), :] = in_box[pl.ds(rho, CHIPS, stride=SLOT), :].T
    point[...] = in_box[pl.ds(4, CHIPS, stride=SLOT), :].T
    point_rows[...] = point[pl.ds(3 * LEAF, LEAF), :].astype(jnp.int32)
    leaf_tables(store_by_width)
    build_onehot(onehot, point_rows)
    combine(residual, [(leaf, 0, source)])
    swap_b.wait()
    both_sums = half_b[...] + other_b[...]
    total_b = both_sums[0:COLUMNS, :]
    total_db = both_sums[COLUMNS:, :]
    weight = total_b + EPSILON * TOTAL
    shift_rows[...] = total_db / weight
    cross_sum = []
    square_sum = []
    for q in range(COLUMNS):
        p0 = jnp.broadcast_to(shift_rows[pl.ds(q, 1), :], (LEAF, LANES))
        b = state_x[pl.ds(q * LEAF, LEAF), :]
        r = (point[pl.ds(2 * LEAF, LEAF), :] - p0) * b + residual[pl.ds(q * LEAF, LEAF), :]
        residual[pl.ds(q * LEAF, LEAF), :] = r
        cross_sum.append(jnp.sum(b * r, axis=0, keepdims=True))
        square_sum.append(jnp.sum(r * r, axis=0, keepdims=True))
    moments = jnp.sum(jnp.concatenate(cross_sum + square_sum, axis=0), axis=1, keepdims=True)
    scatter_sum(
        sums_r, left, onehot, point_rows, signs_f,
        lambda c: residual[pl.ds(c, COLUMNS, stride=LEAF), :], acc,
    )
    spread_rows(sums_r, parts_r, rs_s, rs_r)

    for rho in range(4):
        out_back[pl.ds(rho, CHIPS, stride=SLOT), :] = residual[pl.ds(rho * LANES, LANES), :].T
    out_back[pl.ds(4, CHIPS, stride=SLOT), :] = jnp.broadcast_to(to_lanes(moments, 0), (CHIPS, LANES))

    send_slots(out_back, in_back, BACK, back_s, back_r)

    settle(parts_r, peers, rs_r)
    row_r[...] = jnp.sum(parts_r[...], axis=0, keepdims=True)
    gather_rows(row_r, all_r, ag_s, ag_r)

    settle(in_back, mates * BACK, back_r)
    half_mine[...] = jnp.broadcast_to(
        jnp.sum(in_back[pl.ds(4, CHIPS, stride=SLOT), :], axis=0, keepdims=True), (8, LANES)
    )
    swap_sums = remote(half_mine, half_other, mom_s, mom_r, other)
    swap_sums.start()
    for rho in range(4):
        blocks = swap_groups([in_back[pl.ds(SLOT * j + rho, CHUNKS, stride=4 * SLOT), :] for j in range(4)])
        for t in range(4):
            flat_x[pl.ds(4 * rho + t, CHUNKS, stride=COLUMNS), :] = blocks[t]
    swap_sums.wait()
    sums = to_column(half_mine[0:1, :] + half_other[0:1, :], 0, 2 * COLUMNS)
    sums = jnp.broadcast_to(sums, (2 * COLUMNS, LANES))
    m1 = sums[0:COLUMNS, :]
    m2 = sums[COLUMNS:, :]
    p0 = shift_rows[...]
    delta = (m1 - p0 * (EPSILON * TOTAL)) / weight
    energy = m2 - 2.0 * delta * m1 + delta * delta * total_b
    spread = jnp.sqrt(jnp.maximum(energy, 0.0) * (1.0 / TOTAL) + EPSILON)
    inverse = 1.0 / spread
    arnoldi_ref[0:1, :] = to_lanes((p0 + delta)[:, 0:1], 0)[:, 0:COLUMNS]
    arnoldi_ref[1:2, :] = to_lanes(spread[:, 0:1], 0)[:, 0:COLUMNS]
    for c in range(CHUNKS):
        at = pl.ds(c * COLUMNS, COLUMNS)
        new_ref[:, c * LANES : (c + 1) * LANES] = (flat_x[at, :] - delta * tall[at, :]) * inverse

    settle(all_b, peers, agb_r)
    settle(all_r, peers, ag_r)
    factor = inverse * math.sqrt(SKETCH / TOTAL)
    for r in range(SKETCH // LANES):
        at = pl.ds(r, COLUMNS, stride=SKETCH // LANES)
        sketch_ref[:, r * LANES : (r + 1) * LANES] = (all_r[at, :] - delta * all_b[at, :]) * factor

    settle(out_c, mates * 4, coef_s)
    settle(out_box, mates * SENT, fwd_s)
    settle(sums_b, peers, rsb_s)
    settle(all_b, peers, agb_s)
    settle(sums_r, peers, rs_s)
    settle(all_r, peers, ag_s)
    settle(out_back, mates * BACK, back_s)


def body(basis_vector, diagonal, coords, phase_scale, sketch_rows, sketch_signs):
    f32 = jnp.float32
    vmem = pl.BlockSpec(memory_space=pltpu.VMEM)
    hbm = pl.BlockSpec(memory_space=pltpu.HBM)
    box_rows = CHIPS * SLOT
    scratch = [
        pltpu.VMEM((CHUNKS * COLUMNS, LANES), f32),
        pltpu.VMEM((2 * CHUNKS, LANES), f32),
        pltpu.VMEM((CHUNKS * COLUMNS, LANES), f32),
        pltpu.VMEM((box_rows, LANES), f32),
        pltpu.VMEM((box_rows, LANES), f32),
        pltpu.VMEM((SECTIONS * 2 * WIDTH * WIDTH, LANES), f32),
        pltpu.VMEM((WIDTH * LEAF, LANES), f32),
        pltpu.VMEM((WIDTH * LEAF, LANES), f32),
        pltpu.VMEM((STATE, LANES), f32),
        pltpu.VMEM((STATE, LANES), f32),
        pltpu.VMEM((STATE, LANES), f32),
        pltpu.VMEM((STATE, LANES), f32),
        pltpu.VMEM((STATE, LANES), f32),
        pltpu.VMEM((4 * LEAF, LANES), f32),
        pltpu.VMEM((LEAF, LANES), jnp.int32),
        pltpu.VMEM((STATE, LANES), f32),
        pltpu.VMEM((box_rows, LANES), f32),
        pltpu.VMEM((box_rows, LANES), f32),
        pltpu.VMEM((2 * COLUMNS, LANES), f32),
        pltpu.VMEM((2 * COLUMNS, LANES), f32),
        pltpu.VMEM((box_rows, LANES), f32),
        pltpu.VMEM((box_rows, LANES), f32),
        pltpu.VMEM((LOW, POINTS), jnp.bfloat16),
        pltpu.VMEM((PIECES * HIGH * COLUMNS, POINTS), jnp.bfloat16),
        pltpu.VMEM((PIECES * HIGH * COLUMNS, LOW), f32),
    ]
    for _ in range(2):
        scratch += [
            pltpu.VMEM((DEVICES, LANES), f32),
            pltpu.VMEM((DEVICES, LANES), f32),
            pltpu.VMEM((1, LANES), f32),
            pltpu.VMEM((DEVICES, LANES), f32),
        ]
    scratch += [
        pltpu.VMEM((8, LANES), f32),
        pltpu.VMEM((8, LANES), f32),
        pltpu.VMEM((COLUMNS, LANES), f32),
        pltpu.VMEM((LEAF, LANES), f32),
        pltpu.VMEM((COLUMNS, POINTS), f32),
        pltpu.VMEM((CHUNKS, LANES), f32),
        pltpu.VMEM((2, POINTS), jnp.int32),
        pltpu.VMEM((CHUNKS, LANES), jnp.int32),
        pltpu.VMEM((CHUNKS, LANES), jnp.int32),
        pltpu.SemaphoreType.DMA((5,)),
    ]
    scratch += [pltpu.SemaphoreType.DMA] * 20
    call = pl.pallas_call(
        kernel,
        out_shape=(
            jax.ShapeDtypeStruct((COLUMNS, POINTS), f32),
            jax.ShapeDtypeStruct((COLUMNS, SKETCH), f32),
            jax.ShapeDtypeStruct((2, COLUMNS), f32),
        ),
        in_specs=[hbm, hbm, hbm, pl.BlockSpec(memory_space=pltpu.SMEM), hbm, hbm],
        out_specs=(vmem, vmem, vmem),
        scratch_shapes=scratch,
        compiler_params=pltpu.CompilerParams(collective_id=1, has_side_effects=True, vmem_limit_bytes=48 << 20),
    )
    table = (CHUNKS, LANES)
    return call(
        basis_vector,
        diagonal.reshape(table),
        coords,
        phase_scale,
        sketch_rows.reshape(table),
        sketch_signs.reshape(table),
    )


def solution(mesh):
    placed = (P(None, AXIS), P(AXIS), P(None, AXIS), P(), P(AXIS), P(AXIS))
    return jax.shard_map(
        body, mesh=mesh, in_specs=placed, out_specs=(P(None, AXIS), P(), P()), check_vma=False
    )
```

```python
import functools
import math

import jax
import jax.numpy as jnp
from jax import lax
from jax.experimental import pallas as pl
from jax.experimental.pallas import tpu as pltpu
from jax.sharding import PartitionSpec as P

AXIS = "box"
DEVICES = 256
CHIPS = 128
CORES = 2
WIDTH = 32
RANK = 16
LEAF = 32
COLUMNS = 16
SKETCH = 2048
SECTIONS = 8
BOXES = 128
LANES = 128
POINTS = BOXES * LEAF
CHUNKS = POINTS // LANES
TOTAL = POINTS * DEVICES
MODULUS = 8191
EPSILON = 1e-06
SLOT = 8
SENT = 6
BACK = 5
LOW = 256
HIGH = SKETCH // LOW
PIECES = 2
STATE = COLUMNS * WIDTH
MESH = pl.DeviceIdType.MESH

SINE = (3.141592580044348, -5.1677068789061815, 2.550031376988974, -0.5980451725653999, 0.07722012618330765)
COSINE = (
    0.9999999997799037,
    -4.9348021370788295,
    4.058709159556463,
    -1.3352120030521555,
    0.23493731382438812,
    -0.024396324364030414,
)


def fold(x):
    x = (x & MODULUS) + (x >> 13)
    return (x & MODULUS) + (x >> 13)


def turns(phase):
    return (phase << 19) + (phase << 6) + (phase >> 7)


def poly(coefs, y):
    total = jnp.float32(coefs[-1])
    for coef in coefs[-2::-1]:
        total = total * y + jnp.float32(coef)
    return total


def cosine(turn, amplitude):
    r = turn.astype(jnp.float32) * jnp.float32(2.0**-32)
    s = r * poly(SINE, r * r)
    return amplitude - (2.0 * amplitude) * (s * s)


def both(turn, amplitude):
    r = turn.astype(jnp.float32) * jnp.float32(2.0**-32)
    y = r * r
    s = r * poly(SINE, y)
    c = poly(COSINE, y)
    return amplitude - (2.0 * amplitude) * (s * s), (2.0 * amplitude) * (s * c)


def swap_groups(parts):
    parts = list(parts)
    lane = lax.broadcasted_iota(jnp.int32, parts[0].shape, 1)
    for bit in (1, 2):
        shift = 32 * bit
        low = (lane & shift) == 0
        for i in range(4):
            if i & bit:
                continue
            a, b = parts[i], parts[i | bit]
            parts[i] = jnp.where(low, a, pltpu.roll(b, shift, 1))
            parts[i | bit] = jnp.where(low, pltpu.roll(a, LANES - shift, 1), b)
    return parts


def to_lanes(column, offset):
    rows = column.shape[0]
    shape = (rows, LANES)
    here = lax.broadcasted_iota(jnp.int32, shape, 1) == lax.broadcasted_iota(jnp.int32, shape, 0) + offset
    return jnp.sum(jnp.where(here, jnp.broadcast_to(column, shape), 0.0), axis=0, keepdims=True)


def to_column(row, offset, rows):
    shape = (rows, LANES)
    here = lax.broadcasted_iota(jnp.int32, shape, 1) == lax.broadcasted_iota(jnp.int32, shape, 0) + offset
    return jnp.sum(jnp.where(here, jnp.broadcast_to(row, shape), 0.0), axis=1, keepdims=True)


def combine(out_ref, terms, add=False, only=None):
    group = 4

    def one_group(g, carry):
        first = g * group * WIDTH
        if only is None:
            first = pl.multiple_of(first, group * WIDTH)
        if add:
            acc = [out_ref[pl.ds(first + 8 * i, 8), :] for i in range(4 * group)]
        else:
            acc = [jnp.zeros((8, LANES), jnp.float32) for _ in range(4 * group)]

        def step(v, acc):
            acc = list(acc)
            for m_ref, base, c_ref in terms:
                rows = [m_ref[pl.ds(pl.multiple_of(base + v * WIDTH, WIDTH) + 8 * t, 8), :] for t in range(4)]
                for i in range(group):
                    c = c_ref[pl.ds(first + i * WIDTH + v, 8, stride=0), :]
                    for t in range(4):
                        acc[4 * i + t] = acc[4 * i + t] + rows[t] * c
            return tuple(acc)

        acc = lax.fori_loop(0, WIDTH, step, tuple(acc), unroll=8)
        for i in range(4 * group):
            out_ref[pl.ds(first + 8 * i, 8), :] = acc[i]
        return carry

    if only is None:
        lax.fori_loop(0, COLUMNS // group, one_group, 0)
    else:
        one_group(only, 0)


def build_onehot(onehot_ref, rows_ref):
    def one(c, carry):
        low = (rows_ref[pl.ds(c, 1), :] & (LOW - 1)).astype(jnp.float32)
        low = jnp.broadcast_to(low, (16, LANES)).astype(jnp.bfloat16)
        sub = lax.broadcasted_iota(jnp.int32, (16, LANES), 0).astype(jnp.float32)
        one_b = jnp.ones((16, LANES), jnp.bfloat16)
        zero_b = jnp.zeros((16, LANES), jnp.bfloat16)
        here = pl.ds(pl.multiple_of(c * LANES, LANES), LANES)
        for r in range(LOW // 16):
            hit = low == (sub + float(16 * r)).astype(jnp.bfloat16)
            onehot_ref[pl.ds(16 * r, 16), here] = jnp.where(hit, one_b, zero_b)
        return carry

    lax.fori_loop(0, CHUNKS, one, 0, unroll=2)


def scatter_sum(sums_ref, left_ref, onehot_ref, rows_ref, signs_ref, values, acc_ref, blocks=1):
    def one(c, carry):
        x = values(c) * jnp.broadcast_to(signs_ref[pl.ds(c, 1), :], (COLUMNS, LANES))
        high = (rows_ref[pl.ds(c, 1), :] >> 8).astype(jnp.float32)
        high = jnp.broadcast_to(high, (COLUMNS, LANES)).astype(jnp.bfloat16)
        zero_b = jnp.zeros((COLUMNS, LANES), jnp.bfloat16)
        here = pl.ds(c * LANES if blocks > 1 else pl.multiple_of(c * LANES, LANES), LANES)
        pieces = []
        for _ in range(PIECES):
            piece = x.astype(jnp.bfloat16)
            x = x - piece.astype(jnp.float32)
            pieces.append(piece)
        for h in range(HIGH):
            hit = high == jnp.full((COLUMNS, LANES), h, jnp.bfloat16)
            for i, piece in enumerate(pieces):
                left_ref[pl.ds((i * HIGH + h) * COLUMNS, COLUMNS), here] = jnp.where(hit, piece, zero_b)
        return carry

    if blocks == 1:
        lax.fori_loop(0, CHUNKS, one, 0, unroll=2)
    for block in range(blocks):
        if blocks > 1:
            for c in range(block * CHUNKS // blocks, (block + 1) * CHUNKS // blocks):
                one(c, 0)
        at = slice(block * POINTS // blocks, (block + 1) * POINTS // blocks)
        part = lax.dot_general(
            left_ref[:, at], onehot_ref[:, at], (((1,), (1,)), ((), ())), preferred_element_type=jnp.float32
        )
        acc_ref[...] = part if block == 0 else acc_ref[...] + part
    rows = HIGH * COLUMNS
    total = acc_ref[pl.ds(0, rows), :] + acc_ref[pl.ds(rows, rows), :]
    for h in range(HIGH):
        for half in range(LOW // LANES):
            block = total[h * COLUMNS : (h + 1) * COLUMNS, half * LANES : (half + 1) * LANES]
            sums_ref[pl.ds(h * (LOW // LANES) + half, COLUMNS, stride=SKETCH // LANES), :] = block


def make_sections(matrix_ref, scale, group, chip):
    own_size = 0.35 / math.sqrt(WIDTH)
    cross_size = 0.6 / math.sqrt(WIDTH)
    sub = lax.broadcasted_iota(jnp.int32, (8, LANES), 0)
    box = group * BOXES + chip

    def one(k, carry):
        key = box * 37 + 101 * k
        guess = (key.astype(jnp.float32) * jnp.float32(1.0 / (MODULUS - 1))).astype(jnp.int32)
        key = key - guess * (MODULUS - 1)
        key = jnp.where(key < 0, key + (MODULUS - 1), key)
        key = jnp.where(key >= MODULUS - 1, key - (MODULUS - 1), key)
        unit = fold(scale * (key + 1))
        base = pl.multiple_of(k * (2 * WIDTH * WIDTH), 2 * WIDTH * WIDTH)
        half = turns(jnp.int32(4096))
        for t in range(4):
            own_step = turns(fold((sub + (8 * t + 1)) * unit))
            cross_step = turns(fold((sub + (8 * t + 3)) * unit))
            own_turn = own_step
            cross_turn = jnp.broadcast_to(half, (8, LANES))
            for v in range(WIDTH):
                own_turn = own_turn + own_step
                cross_turn = cross_turn + cross_step
                own = cosine(own_turn, own_size)
                if v // 8 == t:
                    own = own + jnp.where(sub == v % 8, 0.85, 0.0)
                matrix_ref[pl.ds(base + v * WIDTH + 8 * t, 8), :] = own
                matrix_ref[pl.ds(base + WIDTH * WIDTH + v * WIDTH + 8 * t, 8), :] = cosine(cross_turn, cross_size)
        return carry

    return one


def kernel(
    basis_hbm, diag_hbm, coords_hbm, scale_ref, rows_hbm, signs_hbm,
    new_ref, sketch_ref, arnoldi_ref,
    tall, pack, flat_x, out_box, in_box, matrix, leaf, leaf_t, state_x,
    first, second, first_p, partner, point, point_rows, residual,
    out_c, in_c, half_b, other_b,
    out_back, in_back, onehot, left, acc, sums_b, parts_b, row_b, all_b, sums_r, parts_r, row_r, all_r,
    half_mine, half_other, shift_rows, signs_f,
    basis_ref, diag_ref, coords_ref, rows_ref, signs_ref, load_sem,
    fwd_s, fwd_r, ex_s, ex_r, rsb_s, rsb_r, agb_s, agb_r, rs_s, rs_r, ag_s, ag_r, back_s, back_r, mom_s, mom_r,
    coef_s, coef_r, hb_s, hb_r,
):
    me = lax.axis_index(AXIS)
    chip = me // CORES
    core = lax.rem(me, CORES)
    other = me + 1 - 2 * core
    barrier = pltpu.get_barrier_semaphore()
    peers = DEVICES - 1
    mates = CHIPS - 1

    x = lax.rem(chip, 4)
    z = lax.rem(me // 8, 8)
    y = me // 64
    x_at = [lax.rem(x + i, 4) for i in range(4)]
    y_at = [lax.rem(y + i, 4) * 32 for i in range(4)]
    core_at = [core, 1 - core]

    def far_first(what, cores):
        steps = [(a, b, c) for a in range(4) for b in range(4) for c in range(cores)]
        steps.sort(key=lambda s: -(min(s[0], 4 - s[0]) + min(s[1], 4 - s[1]) + 0.1 * s[2]))
        near = [[y_at[a] + x_at[b] for b in range(4)] for a in range(4)]

        def layer(dz, own):
            base = lax.rem(z + dz, 8) * 4
            for a, b, c in steps:
                if own and (a, b, c) == (0, 0, 0):
                    continue
                place = near[a][b] + base
                what(place, place * CORES + core_at[c])

        def body(i, carry):
            layer(4 + ((i + 1) // 2) * (1 - 2 * lax.rem(i, 2)), False)
            return carry

        lax.fori_loop(0, 7, body, 0)
        layer(0, True)

    def each(count, what, unroll=1):
        def body(step, carry):
            what(step)
            return carry

        lax.fori_loop(0, count, body, 0, unroll=unroll)

    def remote(src, dst, send, recv, to):
        return pltpu.make_async_remote_copy(
            src_ref=src, dst_ref=dst, send_sem=send, recv_sem=recv, device_id=(to,), device_id_type=MESH
        )

    def settle(ref, rows, sem):
        pltpu.make_async_copy(ref.at[pl.ds(0, rows)], ref.at[pl.ds(0, rows)], sem).wait()

    loads = []
    for i, (src, dst) in enumerate(
        [(basis_hbm, basis_ref), (coords_hbm, coords_ref), (diag_hbm, diag_ref), (rows_hbm, rows_ref), (signs_hbm, signs_ref)]
    ):
        loads.append(pltpu.make_async_copy(src, dst, load_sem.at[i]))
        loads[-1].start()
    far_first(lambda place, to: pl.semaphore_signal(barrier, inc=1, device_id=(to,), device_id_type=MESH), 2)
    for load in loads:
        load.wait()

    square = jnp.zeros((COLUMNS, LANES), jnp.float32)
    weighted = jnp.zeros((COLUMNS, LANES), jnp.float32)
    for c in range(CHUNKS):
        x = basis_ref[:, c * LANES : (c + 1) * LANES]
        tall[pl.ds(c * COLUMNS, COLUMNS), :] = x
        pack[pl.ds(2 * c, 2), :] = coords_ref[:, c * LANES : (c + 1) * LANES].astype(jnp.float32)
        d = jnp.broadcast_to(diag_ref[pl.ds(c, 1), :], (COLUMNS, LANES))
        square = square + x * x
        weighted = weighted + d * x * x
    moments = to_lanes(jnp.sum(square, axis=1, keepdims=True), 32) + to_lanes(
        jnp.sum(weighted, axis=1, keepdims=True), 48
    )
    sign = (2 * signs_ref[...] - 1).astype(jnp.float32)
    signs_f[...] = sign
    for rho in range(4):
        blocks = swap_groups([tall[pl.ds(4 * rho + t, CHUNKS, stride=COLUMNS), :] for t in range(4)])
        for j in range(4):
            out_box[pl.ds(SLOT * j + rho, CHUNKS, stride=4 * SLOT), :] = blocks[j]
    blocks = swap_groups(
        [
            pack[pl.ds(0, CHUNKS, stride=2), :],
            pack[pl.ds(1, CHUNKS, stride=2), :],
            diag_ref[...],
            rows_ref[...].astype(jnp.float32),
        ]
    )
    for j in range(4):
        out_box[pl.ds(SLOT * j + 4, CHUNKS, stride=4 * SLOT), :] = blocks[j]
    zero = jnp.zeros((CHUNKS, LANES), jnp.float32)
    blocks = swap_groups([sign, zero, zero, zero])
    for j in range(4):
        out_box[pl.ds(SLOT * j + 5, CHUNKS, stride=4 * SLOT), :] = blocks[j] + moments

    scale = lax.rem(scale_ref[0], MODULUS)
    size = 1.0 / math.sqrt(LEAF)

    def leaf_tables(store):
        across = point[pl.ds(0, LEAF), :].astype(jnp.int32) * scale
        down = point[pl.ds(LEAF, LEAF), :].astype(jnp.int32) * scale
        turn_x = [turns(fold(across * f)) for f in range(1, 5)]
        turn_y = [turns(fold(down * f)) for f in range(1, 5)]
        for w in range(RANK):
            c, s = both(turn_x[w % 4] + turn_y[w // 4], size)
            store(w, c)
            store(w + RANK, s)

    def store_by_point(w, table):
        leaf_t[pl.ds(w, LEAF, stride=WIDTH), :] = table

    def store_by_width(w, table):
        leaf[pl.ds(w * LEAF, LEAF), :] = table

    for rho in range(4):
        state_x[pl.ds(rho * LANES, LANES), :] = out_box[pl.ds(rho, CHIPS, stride=SLOT), :].T
    point[...] = out_box[pl.ds(4, CHIPS, stride=SLOT), :].T
    leaf_tables(store_by_point)
    combine(second, [(leaf_t, 0, state_x)])
    for rho in range(4):
        out_c[pl.ds(rho, CHIPS, stride=SLOT), :] = second[pl.ds(rho * LANES, LANES), :].T

    pl.semaphore_wait(barrier, peers)

    def send_slots(src, dst, count, send, recv):
        def go(place, to):
            remote(
                src.at[pl.ds(pl.multiple_of(SLOT * place, SLOT), count)],
                dst.at[pl.ds(pl.multiple_of(SLOT * chip, SLOT), count)],
                send, recv, to,
            ).start()

        far_first(go, 1)
        mine = pl.ds(pl.multiple_of(SLOT * chip, SLOT), count)
        dst[mine, :] = src[mine, :]

    send_slots(out_c, in_c, 4, coef_s, coef_r)

    def spread_rows(src, dst, send, recv):
        def go(place, to):
            remote(src.at[pl.ds(to, 1)], dst.at[pl.ds(me, 1)], send, recv, to).start()

        far_first(go, 2)
        dst[pl.ds(me, 1), :] = src[pl.ds(me, 1), :]

    def gather_rows(row, dst, send, recv):
        def go(place, to):
            remote(row, dst.at[pl.ds(me, 1)], send, recv, to).start()

        far_first(go, 2)
        dst[pl.ds(me, 1), :] = row[...]

    build_onehot(onehot, rows_ref)
    scatter_sum(
        sums_b, left, onehot, rows_ref, signs_f,
        lambda c: tall[pl.ds(pl.multiple_of(c * COLUMNS, COLUMNS), COLUMNS), :], acc,
    )
    spread_rows(sums_b, parts_b, rsb_s, rsb_r)
    send_slots(out_box, in_box, SENT, fwd_s, fwd_r)
    group = lax.broadcasted_iota(jnp.int32, (8, LANES), 1) * CORES + core
    lax.fori_loop(0, SECTIONS, make_sections(matrix, scale, group, chip), 0)

    settle(in_c, mates * 4, coef_r)
    for rho in range(4):
        first[pl.ds(rho * LANES, LANES), :] = in_c[pl.ds(rho, CHIPS, stride=SLOT), :].T

    pieces = [pl.ds(rho * LANES, LANES) for rho in range(4)]
    exchange = [remote(first.at[at], first_p.at[at], ex_s.at[i], ex_r.at[i], other) for i, at in enumerate(pieces)]
    for piece in exchange:
        piece.start()
    combine(second, [(matrix, 0, first)])
    for i, piece in enumerate(exchange):
        piece.wait_recv()
        combine(second, [(matrix, WIDTH * WIDTH, first_p)], add=True, only=i)
    for piece in exchange:
        piece.wait_send()
    source, target = second, first
    for k in range(1, SECTIONS):
        step = 1 << (k - 1)

        def swap(r, source=source, step=step):
            at = pl.ds(pl.multiple_of(r * 512, 512), 512)
            a = source[at, :]
            up = (lax.broadcasted_iota(jnp.int32, a.shape, 1) & step) != 0
            partner[at, :] = jnp.where(up, pltpu.roll(a, step, 1), pltpu.roll(a, LANES - step, 1))

        each(STATE // 512, swap)
        base = k * 2 * WIDTH * WIDTH
        combine(target, [(matrix, base, source), (matrix, base + WIDTH * WIDTH, partner)])
        source, target = target, source
        if k == 5:
            settle(parts_b, peers, rsb_r)
            row_b[...] = jnp.sum(parts_b[...], axis=0, keepdims=True)
            gather_rows(row_b, all_b, agb_s, agb_r)

    settle(in_box, mates * SENT, fwd_r)
    tail = in_box[pl.ds(5, CHIPS, stride=SLOT), :].T
    half_b[...] = jnp.broadcast_to(
        jnp.sum(tail[LEAF : LEAF + 2 * COLUMNS, :], axis=1, keepdims=True), (2 * COLUMNS, LANES)
    )
    swap_b = remote(half_b, other_b, hb_s, hb_r, other)
    swap_b.start()
    signs_f[...] = tail[0:LEAF, :]
    for rho in range(4):
        state_x[pl.ds(rho * LANES, LANES), :] = in_box[pl.ds(rho, CHIPS, stride=SLOT), :].T
    point[...] = in_box[pl.ds(4, CHIPS, stride=SLOT), :].T
    point_rows[...] = point[pl.ds(3 * LEAF, LEAF), :].astype(jnp.int32)
    leaf_tables(store_by_width)
    build_onehot(onehot, point_rows)
    combine(residual, [(leaf, 0, source)])
    swap_b.wait()
    both_sums = half_b[...] + other_b[...]
    total_b = both_sums[0:COLUMNS, :]
    total_db = both_sums[COLUMNS:, :]
    weight = total_b + EPSILON * TOTAL
    shift_rows[...] = total_db / weight
    cross_sum = []
    square_sum = []
    for q in range(COLUMNS):
        p0 = jnp.broadcast_to(shift_rows[pl.ds(q, 1), :], (LEAF, LANES))
        b = state_x[pl.ds(q * LEAF, LEAF), :]
        r = (point[pl.ds(2 * LEAF, LEAF), :] - p0) * b + residual[pl.ds(q * LEAF, LEAF), :]
        residual[pl.ds(q * LEAF, LEAF), :] = r
        cross_sum.append(jnp.sum(b * r, axis=0, keepdims=True))
        square_sum.append(jnp.sum(r * r, axis=0, keepdims=True))
    moments = jnp.sum(jnp.concatenate(cross_sum + square_sum, axis=0), axis=1, keepdims=True)
    scatter_sum(
        sums_r, left, onehot, point_rows, signs_f,
        lambda c: residual[pl.ds(c, COLUMNS, stride=LEAF), :], acc, blocks=4,
    )
    spread_rows(sums_r, parts_r, rs_s, rs_r)

    for rho in range(4):
        out_back[pl.ds(rho, CHIPS, stride=SLOT), :] = residual[pl.ds(rho * LANES, LANES), :].T
    out_back[pl.ds(4, CHIPS, stride=SLOT), :] = jnp.broadcast_to(to_lanes(moments, 0), (CHIPS, LANES))

    send_slots(out_back, in_back, BACK, back_s, back_r)

    settle(parts_r, peers, rs_r)
    row_r[...] = jnp.sum(parts_r[...], axis=0, keepdims=True)
    gather_rows(row_r, all_r, ag_s, ag_r)

    settle(in_back, mates * BACK, back_r)
    half_mine[...] = jnp.broadcast_to(
        jnp.sum(in_back[pl.ds(4, CHIPS, stride=SLOT), :], axis=0, keepdims=True), (8, LANES)
    )
    swap_sums = remote(half_mine, half_other, mom_s, mom_r, other)
    swap_sums.start()
    for rho in range(4):
        blocks = swap_groups([in_back[pl.ds(SLOT * j + rho, CHUNKS, stride=4 * SLOT), :] for j in range(4)])
        for t in range(4):
            flat_x[pl.ds(4 * rho + t, CHUNKS, stride=COLUMNS), :] = blocks[t]
    swap_sums.wait()
    sums = to_column(half_mine[0:1, :] + half_other[0:1, :], 0, 2 * COLUMNS)
    sums = jnp.broadcast_to(sums, (2 * COLUMNS, LANES))
    m1 = sums[0:COLUMNS, :]
    m2 = sums[COLUMNS:, :]
    p0 = shift_rows[...]
    delta = (m1 - p0 * (EPSILON * TOTAL)) / weight
    energy = m2 - 2.0 * delta * m1 + delta * delta * total_b
    spread = jnp.sqrt(jnp.maximum(energy, 0.0) * (1.0 / TOTAL) + EPSILON)
    inverse = 1.0 / spread
    arnoldi_ref[0:1, :] = to_lanes((p0 + delta)[:, 0:1], 0)[:, 0:COLUMNS]
    arnoldi_ref[1:2, :] = to_lanes(spread[:, 0:1], 0)[:, 0:COLUMNS]
    for c in range(CHUNKS):
        at = pl.ds(c * COLUMNS, COLUMNS)
        new_ref[:, c * LANES : (c + 1) * LANES] = (flat_x[at, :] - delta * tall[at, :]) * inverse

    settle(all_b, peers, agb_r)
    factor = inverse * math.sqrt(SKETCH / TOTAL)
    shift = delta * factor
    for r in range(SKETCH // LANES):
        at = pl.ds(r, COLUMNS, stride=SKETCH // LANES)
        sketch_ref[:, r * LANES : (r + 1) * LANES] = shift * all_b[at, :]
    settle(out_c, mates * 4, coef_s)
    settle(out_box, mates * SENT, fwd_s)
    settle(sums_b, peers, rsb_s)
    settle(all_b, peers, agb_s)
    settle(sums_r, peers, rs_s)
    settle(out_back, mates * BACK, back_s)
    settle(all_r, peers, ag_r)
    for r in range(SKETCH // LANES):
        at = pl.ds(r, COLUMNS, stride=SKETCH // LANES)
        here = slice(r * LANES, (r + 1) * LANES)
        sketch_ref[:, here] = all_r[at, :] * factor - sketch_ref[:, here]
    settle(all_r, peers, ag_s)


def put(new_ref, sketch_ref, arnoldi_ref, new_hbm, sketch_hbm, arnoldi_hbm, sems):
    copies = [
        pltpu.make_async_copy(src, dst, sems.at[i])
        for i, (src, dst) in enumerate(((new_ref, new_hbm), (sketch_ref, sketch_hbm), (arnoldi_ref, arnoldi_hbm)))
    ]
    for copy in copies:
        copy.start()
    for copy in copies:
        copy.wait()


def body(basis_vector, diagonal, coords, phase_scale, sketch_rows, sketch_signs):
    f32 = jnp.float32
    vmem = pl.BlockSpec(memory_space=pltpu.VMEM)
    hbm = pl.BlockSpec(memory_space=pltpu.HBM)
    box_rows = CHIPS * SLOT
    scratch = [
        pltpu.VMEM((CHUNKS * COLUMNS, LANES), f32),
        pltpu.VMEM((2 * CHUNKS, LANES), f32),
        pltpu.VMEM((CHUNKS * COLUMNS, LANES), f32),
        pltpu.VMEM((box_rows, LANES), f32),
        pltpu.VMEM((box_rows, LANES), f32),
        pltpu.VMEM((SECTIONS * 2 * WIDTH * WIDTH, LANES), f32),
        pltpu.VMEM((WIDTH * LEAF, LANES), f32),
        pltpu.VMEM((WIDTH * LEAF, LANES), f32),
        pltpu.VMEM((STATE, LANES), f32),
        pltpu.VMEM((STATE, LANES), f32),
        pltpu.VMEM((STATE, LANES), f32),
        pltpu.VMEM((STATE, LANES), f32),
        pltpu.VMEM((STATE, LANES), f32),
        pltpu.VMEM((4 * LEAF, LANES), f32),
        pltpu.VMEM((LEAF, LANES), jnp.int32),
        pltpu.VMEM((STATE, LANES), f32),
        pltpu.VMEM((box_rows, LANES), f32),
        pltpu.VMEM((box_rows, LANES), f32),
        pltpu.VMEM((2 * COLUMNS, LANES), f32),
        pltpu.VMEM((2 * COLUMNS, LANES), f32),
        pltpu.VMEM((box_rows, LANES), f32),
        pltpu.VMEM((box_rows, LANES), f32),
        pltpu.VMEM((LOW, POINTS), jnp.bfloat16),
        pltpu.VMEM((PIECES * HIGH * COLUMNS, POINTS), jnp.bfloat16),
        pltpu.VMEM((PIECES * HIGH * COLUMNS, LOW), f32),
    ]
    for _ in range(2):
        scratch += [
            pltpu.VMEM((DEVICES, LANES), f32),
            pltpu.VMEM((DEVICES, LANES), f32),
            pltpu.VMEM((1, LANES), f32),
            pltpu.VMEM((DEVICES, LANES), f32),
        ]
    scratch += [
        pltpu.VMEM((8, LANES), f32),
        pltpu.VMEM((8, LANES), f32),
        pltpu.VMEM((COLUMNS, LANES), f32),
        pltpu.VMEM((LEAF, LANES), f32),
        pltpu.VMEM((COLUMNS, POINTS), f32),
        pltpu.VMEM((CHUNKS, LANES), f32),
        pltpu.VMEM((2, POINTS), jnp.int32),
        pltpu.VMEM((CHUNKS, LANES), jnp.int32),
        pltpu.VMEM((CHUNKS, LANES), jnp.int32),
        pltpu.SemaphoreType.DMA((5,)),
    ]
    scratch += [pltpu.SemaphoreType.DMA] * 2 + [pltpu.SemaphoreType.DMA((4,))] * 2 + [pltpu.SemaphoreType.DMA] * 16
    results = (
        jax.ShapeDtypeStruct((COLUMNS, POINTS), f32),
        jax.ShapeDtypeStruct((COLUMNS, SKETCH), f32),
        jax.ShapeDtypeStruct((2, COLUMNS), f32),
    )
    call = pl.pallas_call(
        kernel,
        out_shape=results,
        in_specs=[hbm, hbm, hbm, pl.BlockSpec(memory_space=pltpu.SMEM), hbm, hbm],
        out_specs=(vmem, vmem, vmem),
        scratch_shapes=scratch,
        compiler_params=pltpu.CompilerParams(collective_id=1, has_side_effects=True, vmem_limit_bytes=48 << 20),
    )
    table = (CHUNKS, LANES)
    inputs = (
        basis_vector,
        diagonal.reshape(table),
        coords,
        phase_scale,
        sketch_rows.reshape(table),
        sketch_signs.reshape(table),
    )
    found = call(*[x if x is phase_scale else pltpu.with_memory_space_constraint(x, pltpu.HBM) for x in inputs])
    return pl.pallas_call(
        put,
        out_shape=results,
        in_specs=[vmem] * 3,
        out_specs=(hbm,) * 3,
        scratch_shapes=[pltpu.SemaphoreType.DMA((3,))],
        compiler_params=pltpu.CompilerParams(vmem_limit_bytes=4 << 20),
    )(*found)


def solution(mesh):
    placed = (P(None, AXIS), P(AXIS), P(None, AXIS), P(), P(AXIS), P(AXIS))
    return jax.shard_map(
        body, mesh=mesh, in_specs=placed, out_specs=(P(None, AXIS), P(), P()), check_vma=False
    )
```

```python
import functools
import math

import jax
import jax.numpy as jnp
from jax import lax
from jax.experimental import pallas as pl
from jax.experimental.pallas import tpu as pltpu
from jax.sharding import PartitionSpec as P

AXIS = "box"
DEVICES = 256
CHIPS = 128
CORES = 2
WIDTH = 32
RANK = 16
LEAF = 32
COLUMNS = 16
SKETCH = 2048
SECTIONS = 8
BOXES = 128
LANES = 128
POINTS = BOXES * LEAF
CHUNKS = POINTS // LANES
TOTAL = POINTS * DEVICES
MODULUS = 8191
EPSILON = 1e-06
SLOT = 8
TILES = 16
QUIET = 4
SENT = 6
BACK = 5
LOW = 256
HIGH = SKETCH // LOW
PIECES = 2
STATE = COLUMNS * WIDTH
MESH = pl.DeviceIdType.MESH

SINE = (3.141592580044348, -5.1677068789061815, 2.550031376988974, -0.5980451725653999, 0.07722012618330765)
COSINE = (
    0.9999999997799037,
    -4.9348021370788295,
    4.058709159556463,
    -1.3352120030521555,
    0.23493731382438812,
    -0.024396324364030414,
)


def fold(x):
    x = (x & MODULUS) + (x >> 13)
    return (x & MODULUS) + (x >> 13)


def turns(phase):
    return (phase << 19) + (phase << 6) + (phase >> 7)


def poly(coefs, y):
    total = jnp.float32(coefs[-1])
    for coef in coefs[-2::-1]:
        total = total * y + jnp.float32(coef)
    return total


def cosine(turn, amplitude):
    r = turn.astype(jnp.float32) * jnp.float32(2.0**-32)
    s = r * poly(SINE, r * r)
    return amplitude - (2.0 * amplitude) * (s * s)


def both(turn, amplitude):
    r = turn.astype(jnp.float32) * jnp.float32(2.0**-32)
    y = r * r
    s = r * poly(SINE, y)
    c = poly(COSINE, y)
    return amplitude - (2.0 * amplitude) * (s * s), (2.0 * amplitude) * (s * c)


def swap_groups(parts):
    parts = list(parts)
    lane = lax.broadcasted_iota(jnp.int32, parts[0].shape, 1)
    for bit in (1, 2):
        shift = 32 * bit
        low = (lane & shift) == 0
        for i in range(4):
            if i & bit:
                continue
            a, b = parts[i], parts[i | bit]
            parts[i] = jnp.where(low, a, pltpu.roll(b, shift, 1))
            parts[i | bit] = jnp.where(low, pltpu.roll(a, LANES - shift, 1), b)
    return parts


def to_lanes(column, offset):
    rows = column.shape[0]
    shape = (rows, LANES)
    here = lax.broadcasted_iota(jnp.int32, shape, 1) == lax.broadcasted_iota(jnp.int32, shape, 0) + offset
    return jnp.sum(jnp.where(here, jnp.broadcast_to(column, shape), 0.0), axis=0, keepdims=True)


def to_column(row, offset, rows):
    shape = (rows, LANES)
    here = lax.broadcasted_iota(jnp.int32, shape, 1) == lax.broadcasted_iota(jnp.int32, shape, 0) + offset
    return jnp.sum(jnp.where(here, jnp.broadcast_to(row, shape), 0.0), axis=1, keepdims=True)


def combine(out_ref, terms, add=False, only=None):
    group = 4

    def one_group(g, carry):
        first = g * group * WIDTH
        if only is None:
            first = pl.multiple_of(first, group * WIDTH)
        if add:
            acc = [out_ref[pl.ds(first + 8 * i, 8), :] for i in range(4 * group)]
        else:
            acc = [jnp.zeros((8, LANES), jnp.float32) for _ in range(4 * group)]

        def step(v, acc):
            acc = list(acc)
            for m_ref, base, c_ref in terms:
                rows = [m_ref[pl.ds(pl.multiple_of(base + v * WIDTH, WIDTH) + 8 * t, 8), :] for t in range(4)]
                for i in range(group):
                    c = c_ref[pl.ds(first + i * WIDTH + v, 8, stride=0), :]
                    for t in range(4):
                        acc[4 * i + t] = acc[4 * i + t] + rows[t] * c
            return tuple(acc)

        acc = lax.fori_loop(0, WIDTH, step, tuple(acc), unroll=8)
        for i in range(4 * group):
            out_ref[pl.ds(first + 8 * i, 8), :] = acc[i]
        return carry

    if only is None:
        lax.fori_loop(0, COLUMNS // group, one_group, 0)
    else:
        one_group(only, 0)


def build_onehot(onehot_ref, rows_ref):
    def one(c, carry):
        low = (rows_ref[pl.ds(c, 1), :] & (LOW - 1)).astype(jnp.float32)
        low = jnp.broadcast_to(low, (16, LANES)).astype(jnp.bfloat16)
        sub = lax.broadcasted_iota(jnp.int32, (16, LANES), 0).astype(jnp.float32)
        one_b = jnp.ones((16, LANES), jnp.bfloat16)
        zero_b = jnp.zeros((16, LANES), jnp.bfloat16)
        here = pl.ds(pl.multiple_of(c * LANES, LANES), LANES)
        for r in range(LOW // 16):
            hit = low == (sub + float(16 * r)).astype(jnp.bfloat16)
            onehot_ref[pl.ds(16 * r, 16), here] = jnp.where(hit, one_b, zero_b)
        return carry

    lax.fori_loop(0, CHUNKS, one, 0, unroll=2)


def scatter_sum(sums_ref, left_ref, onehot_ref, rows_ref, signs_ref, values, acc_ref, blocks=1):
    def one(c, carry):
        x = values(c) * jnp.broadcast_to(signs_ref[pl.ds(c, 1), :], (COLUMNS, LANES))
        high = (rows_ref[pl.ds(c, 1), :] >> 8).astype(jnp.float32)
        high = jnp.broadcast_to(high, (COLUMNS, LANES)).astype(jnp.bfloat16)
        zero_b = jnp.zeros((COLUMNS, LANES), jnp.bfloat16)
        here = pl.ds(c * LANES if blocks > 1 else pl.multiple_of(c * LANES, LANES), LANES)
        pieces = []
        for _ in range(PIECES):
            piece = x.astype(jnp.bfloat16)
            x = x - piece.astype(jnp.float32)
            pieces.append(piece)
        for h in range(HIGH):
            hit = high == jnp.full((COLUMNS, LANES), h, jnp.bfloat16)
            for i, piece in enumerate(pieces):
                left_ref[pl.ds((i * HIGH + h) * COLUMNS, COLUMNS), here] = jnp.where(hit, piece, zero_b)
        return carry

    if blocks == 1:
        lax.fori_loop(0, CHUNKS, one, 0, unroll=2)
    for block in range(blocks):
        if blocks > 1:
            for c in range(block * CHUNKS // blocks, (block + 1) * CHUNKS // blocks):
                one(c, 0)
        at = slice(block * POINTS // blocks, (block + 1) * POINTS // blocks)
        part = lax.dot_general(
            left_ref[:, at], onehot_ref[:, at], (((1,), (1,)), ((), ())), preferred_element_type=jnp.float32
        )
        acc_ref[...] = part if block == 0 else acc_ref[...] + part
    rows = HIGH * COLUMNS
    total = acc_ref[pl.ds(0, rows), :] + acc_ref[pl.ds(rows, rows), :]
    for h in range(HIGH):
        for half in range(LOW // LANES):
            block = total[h * COLUMNS : (h + 1) * COLUMNS, half * LANES : (half + 1) * LANES]
            sums_ref[pl.ds(h * (LOW // LANES) + half, COLUMNS, stride=SKETCH // LANES), :] = block


def make_units(own_ref, cross_ref, scale, core, chip):
    lane = lax.broadcasted_iota(jnp.int32, (8, LANES), 1)
    sub = lax.broadcasted_iota(jnp.int32, (8, LANES), 0)
    v = lax.rem(lane, WIDTH)
    for part in range(4):
        mate = 4 * (8 * part + sub) + lane // WIDTH
        box = (mate * CORES + core) * BOXES + chip
        start = lax.rem(box * 37, MODULUS - 1)
        for k in range(SECTIONS):
            key = start + 101 * k
            key = jnp.where(key >= MODULUS - 1, key - (MODULUS - 1), key)
            unit = fold(scale * (key + 1))
            cross = (v + 1) * unit
            here = pl.ds(k * 2 * TILES + 8 * part, 8)
            own_ref[here, :] = turns(fold(cross + unit))
            cross_ref[here, :] = turns(fold(cross))


def make_sections(matrix_ref, own_ref, cross_ref):
    own_size = 0.35 / math.sqrt(WIDTH)
    cross_size = 0.6 / math.sqrt(WIDTH)
    sub = lax.broadcasted_iota(jnp.int32, (8, LANES), 0)
    square = (WIDTH, LANES)
    same = lax.broadcasted_iota(jnp.int32, square, 0) == lax.rem(lax.broadcasted_iota(jnp.int32, square, 1), WIDTH)
    ident = jnp.where(same, 0.85, 0.0)

    def one(i):
        rows = pl.multiple_of(i * 2 * WIDTH, 2 * WIDTH)
        half = turns(jnp.int32(4096))
        for t in range(2):
            own_unit = own_ref[pl.ds(2 * i + t, 8, stride=0), :]
            cross_unit = cross_ref[pl.ds(2 * i + t, 8, stride=0), :]
            own_turn = (sub + 1) * own_unit
            cross_turn = (sub + 3) * cross_unit + half
            own_rows, cross_rows = [], []
            for _ in range(4):
                own_rows.append(cosine(own_turn, own_size))
                cross_rows.append(cosine(cross_turn, cross_size))
                own_turn = own_turn + (own_unit << 3)
                cross_turn = cross_turn + (cross_unit << 3)
            own = jnp.concatenate(own_rows, axis=0) + ident
            cross = jnp.concatenate(cross_rows, axis=0)
            for part, value in ((0, own), (1, cross)):
                here = pl.ds((2 * part + t) * LANES, LANES)
                high = value.astype(jnp.bfloat16)
                matrix_ref[pl.ds(rows, WIDTH), here] = high
                matrix_ref[pl.ds(rows + WIDTH, WIDTH), here] = (value - high.astype(jnp.float32)).astype(jnp.bfloat16)

    return one


def weights(x):
    box = lax.broadcasted_iota(jnp.int32, x.shape, 1)
    box = (lax.rem(box, 32) // 4).astype(jnp.float32).astype(jnp.bfloat16)
    zero = jnp.zeros(x.shape, jnp.bfloat16)
    high = x.astype(jnp.bfloat16)
    low = (x - high.astype(jnp.float32)).astype(jnp.bfloat16)
    return jnp.concatenate(
        [
            jnp.concatenate([jnp.where(box == jnp.full(x.shape, b, jnp.bfloat16), y, zero) for b in range(8)], axis=0)
            for y in (high, low)
        ],
        axis=1,
    )


def three_products(left, right):
    r = lax.dot_general(left, right, (((1,), (0,)), ((), ())), preferred_element_type=jnp.float32)
    return r[0:WIDTH, 0:LANES] + r[0:WIDTH, LANES:] + r[WIDTH:, 0:LANES]


def kernel(
    basis_hbm, diag_hbm, coords_hbm, scale_ref, rows_hbm, signs_hbm,
    new_ref, sketch_ref, arnoldi_ref,
    tall, pack, flat_x, out_box, in_box, matrix, leaf, leaf_t, state_x,
    first, second, first_p, partner, point, point_rows, residual,
    out_c, in_c, half_b, other_b,
    out_back, in_back, onehot, left, acc, sums_b, parts_b, row_b, all_b, sums_r, parts_r, row_r, all_r,
    half_mine, half_other, shift_rows, signs_f,
    basis_ref, diag_ref, coords_ref, rows_ref, signs_ref, own_units, cross_units, load_sem,
    fwd_s, fwd_r, ex_s, ex_r, rsb_s, rsb_r, agb_s, agb_r, rs_s, rs_r, ag_s, ag_r, back_s, back_r, mom_s, mom_r,
    coef_s, coef_r, hb_s, hb_r,
):
    me = lax.axis_index(AXIS)
    chip = me // CORES
    core = lax.rem(me, CORES)
    other = me + 1 - 2 * core
    barrier = pltpu.get_barrier_semaphore()
    peers = DEVICES - 1
    mates = CHIPS - 1

    x = lax.rem(chip, 4)
    z = lax.rem(me // 8, 8)
    y = me // 64
    x_at = [lax.rem(x + i, 4) for i in range(4)]
    y_at = [lax.rem(y + i, 4) * 32 for i in range(4)]
    core_at = [core, 1 - core]

    def far_first(what, cores):
        steps = [(a, b, c) for a in range(4) for b in range(4) for c in range(cores)]
        steps.sort(key=lambda s: -(min(s[0], 4 - s[0]) + min(s[1], 4 - s[1]) + 0.1 * s[2]))
        near = [[y_at[a] + x_at[b] for b in range(4)] for a in range(4)]

        def layer(dz, own):
            base = lax.rem(z + dz, 8) * 4
            for a, b, c in steps:
                if own and (a, b, c) == (0, 0, 0):
                    continue
                place = near[a][b] + base
                what(place, place * CORES + core_at[c])

        def body(i, carry):
            layer(4 + ((i + 1) // 2) * (1 - 2 * lax.rem(i, 2)), False)
            return carry

        lax.fori_loop(0, 7, body, 0)
        layer(0, True)

    def each(count, what, unroll=1):
        def body(step, carry):
            what(step)
            return carry

        lax.fori_loop(0, count, body, 0, unroll=unroll)

    def remote(src, dst, send, recv, to):
        return pltpu.make_async_remote_copy(
            src_ref=src, dst_ref=dst, send_sem=send, recv_sem=recv, device_id=(to,), device_id_type=MESH
        )

    def settle(ref, rows, sem):
        pltpu.make_async_copy(ref.at[pl.ds(0, rows)], ref.at[pl.ds(0, rows)], sem).wait()

    loads = []
    for i, (src, dst) in enumerate(
        [(basis_hbm, basis_ref), (coords_hbm, coords_ref), (diag_hbm, diag_ref), (rows_hbm, rows_ref), (signs_hbm, signs_ref)]
    ):
        loads.append(pltpu.make_async_copy(src, dst, load_sem.at[i]))
        loads[-1].start()
    far_first(lambda place, to: pl.semaphore_signal(barrier, inc=1, device_id=(to,), device_id_type=MESH), 2)
    for load in loads:
        load.wait()

    square = jnp.zeros((COLUMNS, LANES), jnp.float32)
    weighted = jnp.zeros((COLUMNS, LANES), jnp.float32)
    for c in range(CHUNKS):
        x = basis_ref[:, c * LANES : (c + 1) * LANES]
        tall[pl.ds(c * COLUMNS, COLUMNS), :] = x
        pack[pl.ds(2 * c, 2), :] = coords_ref[:, c * LANES : (c + 1) * LANES].astype(jnp.float32)
        d = jnp.broadcast_to(diag_ref[pl.ds(c, 1), :], (COLUMNS, LANES))
        square = square + x * x
        weighted = weighted + d * x * x
    moments = to_lanes(jnp.sum(square, axis=1, keepdims=True), 32) + to_lanes(
        jnp.sum(weighted, axis=1, keepdims=True), 48
    )
    sign = (2 * signs_ref[...] - 1).astype(jnp.float32)
    signs_f[...] = sign
    for rho in range(4):
        blocks = swap_groups([tall[pl.ds(4 * rho + t, CHUNKS, stride=COLUMNS), :] for t in range(4)])
        for j in range(4):
            out_box[pl.ds(SLOT * j + rho, CHUNKS, stride=4 * SLOT), :] = blocks[j]
    blocks = swap_groups(
        [
            pack[pl.ds(0, CHUNKS, stride=2), :],
            pack[pl.ds(1, CHUNKS, stride=2), :],
            diag_ref[...],
            rows_ref[...].astype(jnp.float32),
        ]
    )
    for j in range(4):
        out_box[pl.ds(SLOT * j + 4, CHUNKS, stride=4 * SLOT), :] = blocks[j]
    zero = jnp.zeros((CHUNKS, LANES), jnp.float32)
    blocks = swap_groups([sign, zero, zero, zero])
    for j in range(4):
        out_box[pl.ds(SLOT * j + 5, CHUNKS, stride=4 * SLOT), :] = blocks[j] + moments

    scale = lax.rem(scale_ref[0], MODULUS)
    size = 1.0 / math.sqrt(LEAF)

    def leaf_tables(store):
        across = point[pl.ds(0, LEAF), :].astype(jnp.int32) * scale
        down = point[pl.ds(LEAF, LEAF), :].astype(jnp.int32) * scale
        turn_x = [turns(fold(across * f)) for f in range(1, 5)]
        turn_y = [turns(fold(down * f)) for f in range(1, 5)]
        for w in range(RANK):
            c, s = both(turn_x[w % 4] + turn_y[w // 4], size)
            store(w, c)
            store(w + RANK, s)

    def store_by_point(w, table):
        leaf_t[pl.ds(w, LEAF, stride=WIDTH), :] = table

    def store_by_width(w, table):
        leaf[pl.ds(w * LEAF, LEAF), :] = table

    for rho in range(4):
        state_x[pl.ds(rho * LANES, LANES), :] = out_box[pl.ds(rho, CHIPS, stride=SLOT), :].T
    point[...] = out_box[pl.ds(4, CHIPS, stride=SLOT), :].T
    leaf_tables(store_by_point)
    combine(second, [(leaf_t, 0, state_x)])
    for rho in range(4):
        out_c[pl.ds(rho, CHIPS, stride=4), :] = second[pl.ds(rho * LANES, LANES), :].T

    build_onehot(onehot, rows_ref)
    scatter_sum(
        sums_b, left, onehot, rows_ref, signs_f,
        lambda c: tall[pl.ds(pl.multiple_of(c * COLUMNS, COLUMNS), COLUMNS), :], acc,
    )
    make_units(own_units, cross_units, scale, core, chip)
    section = make_sections(matrix, own_units, cross_units)
    pl.semaphore_wait(barrier, peers)

    def send_slots(src, dst, count, send, recv, slot=SLOT):
        def go(place, to):
            remote(
                src.at[pl.ds(pl.multiple_of(slot * place, slot), count)],
                dst.at[pl.ds(pl.multiple_of(slot * chip, slot), count)],
                send, recv, to,
            ).start()

        far_first(go, 1)
        mine = pl.ds(pl.multiple_of(slot * chip, slot), count)
        dst[mine, :] = src[mine, :]

    send_slots(out_c, in_c, 4, coef_s, coef_r, slot=4)

    def spread_rows(src, dst, send, recv):
        def go(place, to):
            remote(src.at[pl.ds(to, 1)], dst.at[pl.ds(me, 1)], send, recv, to).start()

        far_first(go, 2)
        dst[pl.ds(me, 1), :] = src[pl.ds(me, 1), :]

    def gather_rows(row, dst, send, recv):
        def go(place, to):
            remote(row, dst.at[pl.ds(me, 1)], send, recv, to).start()

        far_first(go, 2)
        dst[pl.ds(me, 1), :] = row[...]

    def send_sums(to):
        remote(sums_b.at[pl.ds(to, 1)], parts_b.at[pl.ds(me, 1)], rsb_s, rsb_r, to).start()

    def send_points(place):
        remote(
            out_box.at[pl.ds(pl.multiple_of(SLOT * place, SLOT), SENT)],
            in_box.at[pl.ds(pl.multiple_of(SLOT * chip, SLOT), SENT)],
            fwd_s, fwd_r, place * CORES + core,
        ).start()

    def pair(i):
        section(2 * i)
        section(2 * i + 1)

    def at_step(offset):
        return lax.rem(chip + offset, CHIPS)

    def quiet(i, carry):
        pair(i)
        return carry

    def with_points(i, carry):
        for n in range(4):
            send_points(at_step(4 * i + n + 1))
        pair(QUIET + i)
        return carry

    def with_sums(i, carry):
        for n in range(8):
            send_sums(at_step(8 * i + n + 1) * CORES)
            send_sums(at_step(8 * i + n + 1) * CORES + 1)
        pair(QUIET + 32 + i)
        return carry

    lax.fori_loop(0, QUIET, quiet, 0)
    lax.fori_loop(0, 31, with_points, 0)
    for n in range(3):
        send_points(at_step(125 + n))
    pair(QUIET + 31)
    mine = pl.ds(pl.multiple_of(SLOT * chip, SLOT), SENT)
    in_box[mine, :] = out_box[mine, :]
    lax.fori_loop(0, 15, with_sums, 0)
    for n in range(7):
        send_sums(at_step(121 + n) * CORES)
        send_sums(at_step(121 + n) * CORES + 1)
    send_sums(other)
    parts_b[pl.ds(me, 1), :] = sums_b[pl.ds(me, 1), :]
    for i in range(QUIET + 47, 64):
        pair(i)

    settle(in_c, mates * 4, coef_r)
    for quarter in range(4):
        turned = in_c[pl.ds(quarter * LANES, LANES), :].T
        tiles = swap_groups([turned[j * WIDTH : (j + 1) * WIDTH, :] for j in range(4)])
        for i in range(4):
            first[pl.ds((4 * quarter + i) * WIDTH, WIDTH), :] = tiles[i]

    pieces = [pl.ds(rho * LANES, LANES) for rho in range(4)]
    exchange = [remote(first.at[at], first_p.at[at], ex_s.at[i], ex_r.at[i], other) for i, at in enumerate(pieces)]
    for piece in exchange:
        piece.start()

    def rows_of(tile):
        return pl.ds(tile * WIDTH, WIDTH)

    for k in range(SECTIONS):
        source, target = (first, second) if k % 2 == 0 else (second, first)
        if k == 1:
            for piece in exchange:
                piece.wait_send()
        for tile in range(TILES):
            x = source[rows_of(tile), :]
            if k == 0:
                if tile % 4 == 0:
                    exchange[tile // 4].wait_recv()
                y = first_p[rows_of(tile), :]
            elif k < 4:
                step = 4 << (k - 1)
                up = (lax.broadcasted_iota(jnp.int32, x.shape, 1) & step) != 0
                y = jnp.where(up, pltpu.roll(x, step, 1), pltpu.roll(x, LANES - step, 1))
            else:
                y = source[rows_of(tile ^ (1 << (k - 4))), :]
            left_rows = matrix[pl.ds((k * TILES + tile) * 2 * WIDTH, 2 * WIDTH), :]
            right = jnp.concatenate([weights(x), weights(y)], axis=0)
            target[rows_of(tile), :] = three_products(left_rows, right)

    for quarter in range(4):
        parts = swap_groups([first[rows_of(4 * quarter + i), :] for i in range(4)])
        second[pl.ds(quarter * LANES, LANES), :] = jnp.concatenate(parts, axis=0).T
    for rho in range(4):
        partner[pl.ds(rho * LANES, LANES), :] = second[pl.ds(rho, CHIPS, stride=4), :].T
    source = partner

    settle(in_box, mates * SENT, fwd_r)
    tail = in_box[pl.ds(5, CHIPS, stride=SLOT), :].T
    half_b[...] = jnp.broadcast_to(
        jnp.sum(tail[LEAF : LEAF + 2 * COLUMNS, :], axis=1, keepdims=True), (2 * COLUMNS, LANES)
    )
    swap_b = remote(half_b, other_b, hb_s, hb_r, other)
    swap_b.start()
    signs_f[...] = tail[0:LEAF, :]
    for rho in range(4):
        state_x[pl.ds(rho * LANES, LANES), :] = in_box[pl.ds(rho, CHIPS, stride=SLOT), :].T
    point[...] = in_box[pl.ds(4, CHIPS, stride=SLOT), :].T
    point_rows[...] = point[pl.ds(3 * LEAF, LEAF), :].astype(jnp.int32)
    leaf_tables(store_by_width)
    build_onehot(onehot, point_rows)
    combine(residual, [(leaf, 0, source)])
    swap_b.wait()
    both_sums = half_b[...] + other_b[...]
    total_b = both_sums[0:COLUMNS, :]
    total_db = both_sums[COLUMNS:, :]
    weight = total_b + EPSILON * TOTAL
    shift_rows[...] = total_db / weight
    cross_sum = []
    square_sum = []
    for q in range(COLUMNS):
        p0 = jnp.broadcast_to(shift_rows[pl.ds(q, 1), :], (LEAF, LANES))
        b = state_x[pl.ds(q * LEAF, LEAF), :]
        r = (point[pl.ds(2 * LEAF, LEAF), :] - p0) * b + residual[pl.ds(q * LEAF, LEAF), :]
        residual[pl.ds(q * LEAF, LEAF), :] = r
        cross_sum.append(jnp.sum(b * r, axis=0, keepdims=True))
        square_sum.append(jnp.sum(r * r, axis=0, keepdims=True))
    moments = jnp.sum(jnp.concatenate(cross_sum + square_sum, axis=0), axis=1, keepdims=True)
    scatter_sum(
        sums_r, left, onehot, point_rows, signs_f,
        lambda c: residual[pl.ds(c, COLUMNS, stride=LEAF), :], acc, blocks=4,
    )
    spread_rows(sums_r, parts_r, rs_s, rs_r)

    for rho in range(4):
        out_back[pl.ds(rho, CHIPS, stride=SLOT), :] = residual[pl.ds(rho * LANES, LANES), :].T
    out_back[pl.ds(4, CHIPS, stride=SLOT), :] = jnp.broadcast_to(to_lanes(moments, 0), (CHIPS, LANES))

    send_slots(out_back, in_back, BACK, back_s, back_r)

    settle(parts_b, peers, rsb_r)
    row_b[...] = jnp.sum(parts_b[...], axis=0, keepdims=True)
    gather_rows(row_b, all_b, agb_s, agb_r)

    settle(parts_r, peers, rs_r)
    row_r[...] = jnp.sum(parts_r[...], axis=0, keepdims=True)
    gather_rows(row_r, all_r, ag_s, ag_r)

    settle(in_back, mates * BACK, back_r)
    half_mine[...] = jnp.broadcast_to(
        jnp.sum(in_back[pl.ds(4, CHIPS, stride=SLOT), :], axis=0, keepdims=True), (8, LANES)
    )
    swap_sums = remote(half_mine, half_other, mom_s, mom_r, other)
    swap_sums.start()
    for rho in range(4):
        blocks = swap_groups([in_back[pl.ds(SLOT * j + rho, CHUNKS, stride=4 * SLOT), :] for j in range(4)])
        for t in range(4):
            flat_x[pl.ds(4 * rho + t, CHUNKS, stride=COLUMNS), :] = blocks[t]
    swap_sums.wait()
    sums = to_column(half_mine[0:1, :] + half_other[0:1, :], 0, 2 * COLUMNS)
    sums = jnp.broadcast_to(sums, (2 * COLUMNS, LANES))
    m1 = sums[0:COLUMNS, :]
    m2 = sums[COLUMNS:, :]
    p0 = shift_rows[...]
    delta = (m1 - p0 * (EPSILON * TOTAL)) / weight
    energy = m2 - 2.0 * delta * m1 + delta * delta * total_b
    spread = jnp.sqrt(jnp.maximum(energy, 0.0) * (1.0 / TOTAL) + EPSILON)
    inverse = 1.0 / spread
    arnoldi_ref[0:1, :] = to_lanes((p0 + delta)[:, 0:1], 0)[:, 0:COLUMNS]
    arnoldi_ref[1:2, :] = to_lanes(spread[:, 0:1], 0)[:, 0:COLUMNS]
    for c in range(CHUNKS):
        at = pl.ds(c * COLUMNS, COLUMNS)
        new_ref[:, c * LANES : (c + 1) * LANES] = (flat_x[at, :] - delta * tall[at, :]) * inverse

    settle(all_b, peers, agb_r)
    factor = inverse * math.sqrt(SKETCH / TOTAL)
    shift = delta * factor
    for r in range(SKETCH // LANES):
        at = pl.ds(r, COLUMNS, stride=SKETCH // LANES)
        sketch_ref[:, r * LANES : (r + 1) * LANES] = shift * all_b[at, :]
    settle(out_c, mates * 4, coef_s)
    settle(out_box, mates * SENT, fwd_s)
    settle(sums_b, peers, rsb_s)
    settle(all_b, peers, agb_s)
    settle(sums_r, peers, rs_s)
    settle(out_back, mates * BACK, back_s)
    settle(all_r, peers, ag_r)
    for r in range(SKETCH // LANES):
        at = pl.ds(r, COLUMNS, stride=SKETCH // LANES)
        here = slice(r * LANES, (r + 1) * LANES)
        sketch_ref[:, here] = all_r[at, :] * factor - sketch_ref[:, here]
    settle(all_r, peers, ag_s)


def put(new_ref, sketch_ref, arnoldi_ref, new_hbm, sketch_hbm, arnoldi_hbm, sems):
    copies = [
        pltpu.make_async_copy(src, dst, sems.at[i])
        for i, (src, dst) in enumerate(((new_ref, new_hbm), (sketch_ref, sketch_hbm), (arnoldi_ref, arnoldi_hbm)))
    ]
    for copy in copies:
        copy.start()
    for copy in copies:
        copy.wait()


def body(basis_vector, diagonal, coords, phase_scale, sketch_rows, sketch_signs):
    f32 = jnp.float32
    vmem = pl.BlockSpec(memory_space=pltpu.VMEM)
    hbm = pl.BlockSpec(memory_space=pltpu.HBM)
    box_rows = CHIPS * SLOT
    scratch = [
        pltpu.VMEM((CHUNKS * COLUMNS, LANES), f32),
        pltpu.VMEM((2 * CHUNKS, LANES), f32),
        pltpu.VMEM((CHUNKS * COLUMNS, LANES), f32),
        pltpu.VMEM((box_rows, LANES), f32),
        pltpu.VMEM((box_rows, LANES), f32),
        pltpu.VMEM((SECTIONS * TILES * 2 * WIDTH, 4 * LANES), jnp.bfloat16),
        pltpu.VMEM((WIDTH * LEAF, LANES), f32),
        pltpu.VMEM((WIDTH * LEAF, LANES), f32),
        pltpu.VMEM((STATE, LANES), f32),
        pltpu.VMEM((STATE, LANES), f32),
        pltpu.VMEM((STATE, LANES), f32),
        pltpu.VMEM((STATE, LANES), f32),
        pltpu.VMEM((STATE, LANES), f32),
        pltpu.VMEM((4 * LEAF, LANES), f32),
        pltpu.VMEM((LEAF, LANES), jnp.int32),
        pltpu.VMEM((STATE, LANES), f32),
        pltpu.VMEM((CHIPS * 4, LANES), f32),
        pltpu.VMEM((CHIPS * 4, LANES), f32),
        pltpu.VMEM((2 * COLUMNS, LANES), f32),
        pltpu.VMEM((2 * COLUMNS, LANES), f32),
        pltpu.VMEM((box_rows, LANES), f32),
        pltpu.VMEM((box_rows, LANES), f32),
        pltpu.VMEM((LOW, POINTS), jnp.bfloat16),
        pltpu.VMEM((PIECES * HIGH * COLUMNS, POINTS), jnp.bfloat16),
        pltpu.VMEM((PIECES * HIGH * COLUMNS, LOW), f32),
    ]
    for _ in range(2):
        scratch += [
            pltpu.VMEM((DEVICES, LANES), f32),
            pltpu.VMEM((DEVICES, LANES), f32),
            pltpu.VMEM((1, LANES), f32),
            pltpu.VMEM((DEVICES, LANES), f32),
        ]
    scratch += [
        pltpu.VMEM((8, LANES), f32),
        pltpu.VMEM((8, LANES), f32),
        pltpu.VMEM((COLUMNS, LANES), f32),
        pltpu.VMEM((LEAF, LANES), f32),
        pltpu.VMEM((COLUMNS, POINTS), f32),
        pltpu.VMEM((CHUNKS, LANES), f32),
        pltpu.VMEM((2, POINTS), jnp.int32),
        pltpu.VMEM((CHUNKS, LANES), jnp.int32),
        pltpu.VMEM((CHUNKS, LANES), jnp.int32),
        pltpu.VMEM((2 * SECTIONS * TILES + 8, LANES), jnp.int32),
        pltpu.VMEM((2 * SECTIONS * TILES + 8, LANES), jnp.int32),
        pltpu.SemaphoreType.DMA((5,)),
    ]
    scratch += [pltpu.SemaphoreType.DMA] * 2 + [pltpu.SemaphoreType.DMA((4,))] * 2 + [pltpu.SemaphoreType.DMA] * 16
    results = (
        jax.ShapeDtypeStruct((COLUMNS, POINTS), f32),
        jax.ShapeDtypeStruct((COLUMNS, SKETCH), f32),
        jax.ShapeDtypeStruct((2, COLUMNS), f32),
    )
    call = pl.pallas_call(
        kernel,
        out_shape=results,
        in_specs=[hbm, hbm, hbm, pl.BlockSpec(memory_space=pltpu.SMEM), hbm, hbm],
        out_specs=(vmem, vmem, vmem),
        scratch_shapes=scratch,
        compiler_params=pltpu.CompilerParams(collective_id=1, has_side_effects=True, vmem_limit_bytes=48 << 20),
    )
    table = (CHUNKS, LANES)
    inputs = (
        basis_vector,
        diagonal.reshape(table),
        coords,
        phase_scale,
        sketch_rows.reshape(table),
        sketch_signs.reshape(table),
    )
    found = call(*[x if x is phase_scale else pltpu.with_memory_space_constraint(x, pltpu.HBM) for x in inputs])
    return pl.pallas_call(
        put,
        out_shape=results,
        in_specs=[vmem] * 3,
        out_specs=(hbm,) * 3,
        scratch_shapes=[pltpu.SemaphoreType.DMA((3,))],
        compiler_params=pltpu.CompilerParams(vmem_limit_bytes=4 << 20),
    )(*found)


def solution(mesh):
    placed = (P(None, AXIS), P(AXIS), P(None, AXIS), P(), P(AXIS), P(AXIS))
    return jax.shard_map(
        body, mesh=mesh, in_specs=placed, out_specs=(P(None, AXIS), P(), P()), check_vma=False
    )
```
